32 devices in a mesh: tp: 4 (over z), cp: 8 (over y, x, core).
Axes of the slice: x: 2, y: 2, z: 4, core: 2. Of those that a mesh axis runs over, the one named last changes fastest.
Arguments:
- hidden: bfloat16 [8, 1024, 4096], P(None, 'cp')
- grad_out: bfloat16 [8, 1024, 4096], P(None, 'cp')
- w_query: bfloat16 [4096, 32, 128], P(None, 'tp')
- w_key: bfloat16 [4096, 128], replicated
- w_value: bfloat16 [4096, 128], replicated
- w_out: bfloat16 [32, 128, 4096], P('tp')
Outputs:
- output 1: bfloat16 [8, 1024, 4096], P(None, 'cp')
- output 2: bfloat16 [8, 1024, 4096], P(None, 'cp')
- output 3: float32 [4096, 32, 128], P(None, 'tp')
- output 4: float32 [4096, 128], replicated
- output 5: float32 [4096, 128], replicated
- output 6: float32 [32, 128, 4096], P('tp')
All inputs are finite; a program needn't handle non-finite values.
Results may differ from the reference program's by a relative error of at most 0.0110117.
Values are sent between devices in bfloat16 or wider.
A program may use at most 1 GiB of HBM per device.

```python
import jax
import jax.numpy as jnp
from jax import lax

BATCH = 8
SEQ = 1024
D_MODEL = 4096
HEADS = 32
HEAD_DIM = 128
Q_ROWS = 128


def rope_tables(positions):
    half_dim = HEAD_DIM // 2
    inv_freq = 1.0 / jnp.power(10000.0, jnp.arange(half_dim, dtype=jnp.float32) * (2.0 / HEAD_DIM))
    angles = positions.astype(jnp.float32)[:, None] * inv_freq[None, :]
    return jnp.cos(angles), jnp.sin(angles)


def rotate(rot_in, cos_tab, sin_tab):
    half_dim = rot_in.shape[-1] // 2
    low_half = rot_in[..., :half_dim]
    high_half = rot_in[..., half_dim:]
    return jnp.concatenate([low_half * cos_tab - high_half * sin_tab, high_half * cos_tab + low_half * sin_tab], axis=-1)


def unrotate(rot_in, cos_tab, sin_tab):
    half_dim = rot_in.shape[-1] // 2
    low_half = rot_in[..., :half_dim]
    high_half = rot_in[..., half_dim:]
    return jnp.concatenate([low_half * cos_tab + high_half * sin_tab, high_half * cos_tab - low_half * sin_tab], axis=-1)


def setup_inputs(seed: int = 0) -> dict:
    sub_keys = jax.random.split(jax.random.key(seed), 6)
    hidden = jax.random.normal(sub_keys[0], (BATCH, SEQ, D_MODEL), jnp.float32)
    grad_out = jax.random.normal(sub_keys[1], (BATCH, SEQ, D_MODEL), jnp.float32)
    in_scale = D_MODEL ** -0.5
    w_query = jax.random.normal(sub_keys[2], (D_MODEL, HEADS, HEAD_DIM), jnp.float32) * in_scale
    w_key = jax.random.normal(sub_keys[3], (D_MODEL, HEAD_DIM), jnp.float32) * in_scale
    w_value = jax.random.normal(sub_keys[4], (D_MODEL, HEAD_DIM), jnp.float32) * in_scale
    w_out = jax.random.normal(sub_keys[5], (HEADS, HEAD_DIM, D_MODEL), jnp.float32) * (HEADS * HEAD_DIM) ** -0.5
    return {"hidden": hidden.astype(jnp.bfloat16), "grad_out": grad_out.astype(jnp.bfloat16), "w_query": w_query.astype(jnp.bfloat16), "w_key": w_key.astype(jnp.bfloat16), "w_value": w_value.astype(jnp.bfloat16), "w_out": w_out.astype(jnp.bfloat16)}


def reference(hidden, grad_out, w_query, w_key, w_value, w_out):
    q_scale = HEAD_DIM ** -0.5
    n_blocks = SEQ // Q_ROWS
    cos_tab, sin_tab = rope_tables(jnp.arange(SEQ))
    flat_hidden = hidden.reshape(BATCH * SEQ, D_MODEL)
    key_pre = jnp.dot(flat_hidden, w_key, preferred_element_type=jnp.float32).reshape(BATCH, SEQ, HEAD_DIM)
    key_rot = rotate(key_pre, cos_tab, sin_tab).astype(jnp.bfloat16).astype(jnp.float32)
    val_all = jnp.dot(flat_hidden, w_value, preferred_element_type=jnp.float32).reshape(BATCH, SEQ, HEAD_DIM).astype(jnp.bfloat16).astype(jnp.float32)
    key_pos = jnp.arange(SEQ)
    hid_blocks = hidden.reshape(BATCH, n_blocks, Q_ROWS, D_MODEL).transpose(1, 0, 2, 3)
    grad_blocks = grad_out.reshape(BATCH, n_blocks, Q_ROWS, D_MODEL).transpose(1, 0, 2, 3)
    cos_blocks = cos_tab.reshape(n_blocks, Q_ROWS, HEAD_DIM // 2)
    sin_blocks = sin_tab.reshape(n_blocks, Q_ROWS, HEAD_DIM // 2)
    row_starts = jnp.arange(n_blocks) * Q_ROWS
    kv_zero = jnp.zeros((BATCH, SEQ, HEAD_DIM), jnp.float32)
    big_zero = jnp.zeros((BATCH, SEQ, D_MODEL), jnp.float32)

    def head_step(carry_in, head_weights):
        out_acc, dh_acc, dk_acc, dv_acc = carry_in
        wq_head, wo_head = head_weights

        def block_step(block_carry, block_in):
            dk_run, dv_run, dwq_run, dwo_run = block_carry
            hid_blk, grad_blk, cos_blk, sin_blk, row_start = block_in
            hid_flat = hid_blk.reshape(BATCH * Q_ROWS, D_MODEL)
            grad_flat = grad_blk.reshape(BATCH * Q_ROWS, D_MODEL)
            q_pre = jnp.dot(hid_flat, wq_head, preferred_element_type=jnp.float32).reshape(BATCH, Q_ROWS, HEAD_DIM)
            q_rot = (rotate(q_pre, cos_blk, sin_blk) * q_scale).astype(jnp.bfloat16).astype(jnp.float32)
            scores = jnp.einsum("bqe,bke->bqk", q_rot, key_rot)
            q_pos = row_start + jnp.arange(Q_ROWS)
            allowed = key_pos[None, :] <= q_pos[:, None]
            scores = jnp.where(allowed[None], scores, -jnp.inf)
            probs_blk = jax.nn.softmax(scores, axis=-1)
            attn_blk = jnp.einsum("bqk,bke->bqe", probs_blk, val_all).astype(jnp.bfloat16)
            d_attn = jnp.dot(grad_flat, wo_head.T, preferred_element_type=jnp.float32).astype(jnp.bfloat16)
            attn_f = attn_blk.astype(jnp.float32)
            d_attn_f = d_attn.astype(jnp.float32).reshape(BATCH, Q_ROWS, HEAD_DIM)
            d_prob = jnp.einsum("bqe,bke->bqk", d_attn_f, val_all)
            row_delta = jnp.sum(d_attn_f * attn_f, axis=-1, keepdims=True)
            d_score = probs_blk * (d_prob - row_delta)
            dq_blk = jnp.einsum("bqk,bke->bqe", d_score, key_rot)
            dk_run = dk_run + jnp.einsum("bqk,bqe->bke", d_score, q_rot)
            dv_run = dv_run + jnp.einsum("bqk,bqe->bke", probs_blk, d_attn_f)
            dq_pre = (unrotate(dq_blk, cos_blk, sin_blk) * q_scale).astype(jnp.bfloat16).reshape(BATCH * Q_ROWS, HEAD_DIM)
            attn_flat = attn_blk.reshape(BATCH * Q_ROWS, HEAD_DIM)
            dwq_run = dwq_run + jnp.dot(hid_flat.T, dq_pre, preferred_element_type=jnp.float32)
            dwo_run = dwo_run + jnp.dot(attn_flat.T, grad_flat, preferred_element_type=jnp.float32)
            out_part = jnp.dot(attn_flat, wo_head, preferred_element_type=jnp.float32)
            dh_part = jnp.dot(dq_pre, wq_head.T, preferred_element_type=jnp.float32)
            return (dk_run, dv_run, dwq_run, dwo_run), (out_part, dh_part)

        block_init = (kv_zero, kv_zero, jnp.zeros((D_MODEL, HEAD_DIM), jnp.float32), jnp.zeros((HEAD_DIM, D_MODEL), jnp.float32))
        block_out, block_ys = lax.scan(block_step, block_init, (hid_blocks, grad_blocks, cos_blocks, sin_blocks, row_starts))
        dk_run, dv_run, dwq_run, dwo_run = block_out
        out_parts, dh_parts = block_ys
        out_head = out_parts.reshape(n_blocks, BATCH, Q_ROWS, D_MODEL).transpose(1, 0, 2, 3).reshape(BATCH, SEQ, D_MODEL)
        dh_head = dh_parts.reshape(n_blocks, BATCH, Q_ROWS, D_MODEL).transpose(1, 0, 2, 3).reshape(BATCH, SEQ, D_MODEL)
        new_carry = (out_acc + out_head, dh_acc + dh_head, dk_acc + dk_run, dv_acc + dv_run)
        return new_carry, (dwq_run, dwo_run)

    head_init = (big_zero, big_zero, kv_zero, kv_zero)
    head_out, head_ys = lax.scan(head_step, head_init, (w_query.transpose(1, 0, 2), w_out))
    out_acc, dh_acc, dk_acc, dv_acc = head_out
    d_w_query = head_ys[0].transpose(1, 0, 2)
    d_w_out = head_ys[1]
    dk_pre = unrotate(dk_acc, cos_tab, sin_tab).astype(jnp.bfloat16).reshape(BATCH * SEQ, HEAD_DIM)
    dv_pre = dv_acc.astype(jnp.bfloat16).reshape(BATCH * SEQ, HEAD_DIM)
    d_w_key = jnp.dot(flat_hidden.T, dk_pre, preferred_element_type=jnp.float32)
    d_w_value = jnp.dot(flat_hidden.T, dv_pre, preferred_element_type=jnp.float32)
    dh_kv = jnp.dot(dk_pre, w_key.T, preferred_element_type=jnp.float32) + jnp.dot(dv_pre, w_value.T, preferred_element_type=jnp.float32)
    d_hidden = (dh_acc + dh_kv.reshape(BATCH, SEQ, D_MODEL)).astype(jnp.bfloat16)
    attn_out = out_acc.astype(jnp.bfloat16)
    return attn_out, d_hidden, d_w_query, d_w_key, d_w_value, d_w_out
```

```python
import functools
import jax
import jax.numpy as jnp
from jax import lax
from jax.experimental import pallas as pl
from jax.experimental.pallas import tpu as pltpu
from jax.sharding import PartitionSpec as P

ROWS, DEPTH, LANE, TILE, BRICK, HALF_W = 1024, 4096, 128, 256, 512, 2048
CHIPS, HEADS = 4, 8
VMEM_CAP = 66_000_000
MESH = pl.DeviceIdType.MESH
F32, BF16 = jnp.float32, jnp.bfloat16
NT = (((1,), (1,)), ((), ()))
NN = (((1,), (0,)), ((), ()))
TN = (((0,), (0,)), ((), ()))
ANY = pl.BlockSpec(memory_space=pl.ANY)
VM = pl.BlockSpec(memory_space=pltpu.VMEM)
DMA = pltpu.SemaphoreType.DMA


def dot(lhs, rhs, dims=NN):
    return lax.dot_general(lhs, rhs, dims, preferred_element_type=F32)


def win(index, size):
    start = index * size
    return pl.ds(start if isinstance(start, int) else pl.multiple_of(start, size), size)


def plane_peers(cp):
    x_of = lambda idx: idx + 2 - CHIPS * lax.rem(lax.div(idx, 2), 2)
    y_of = lambda idx: lax.rem(idx + CHIPS, HEADS)
    return x_of(cp), y_of(cp), x_of(y_of(cp)), cp + 1 - 2 * lax.rem(cp, 2)


def hand_over(src, dst, send_sem, recv_sem, tp, cp):
    return pltpu.make_async_remote_copy(src, dst, send_sem, recv_sem, device_id=(tp, cp), device_id_type=MESH)


def rope(tile, cos, sin):
    heads = [tile[:, lo:lo + LANE] for lo in range(0, tile.shape[1], LANE)]
    return [one * cos + pltpu.roll(one, LANE // 2, 1) * sin for one in heads]


def proj_kernel(q_scale, h_ref, g_ref, wq_ref, wo_ref, wk_ref, wv_ref, cos_ref, sin_ref,
                q_out, do_out, kv_out, hbuf, gbuf, wqbuf, wobuf, wkvbuf, qbuf, dobuf, kvbuf,
                load_sem, wkv_sem, osem, send_sem, recv_sem):
    tp, cp = lax.axis_index("tp"), lax.axis_index("cp")
    peers = plane_peers(cp)
    others, partner = peers[:-1], peers[-1]
    barrier = pltpu.get_barrier_semaphore()
    for peer in peers:
        pl.semaphore_signal(barrier, inc=1, device_id=(tp, peer), device_id_type=MESH)
    rows = [win(i, TILE) for i in range(CHIPS)]
    loads_h, loads_g, loads_wq, loads_wo = [
        [pltpu.make_async_copy(src.at[r], dst.at[r], load_sem.at[which, i]) for i, r in enumerate(rows)]
        for which, (src, dst) in enumerate(((h_ref, hbuf), (g_ref, gbuf), (wq_ref, wqbuf), (wo_ref, wobuf)))]
    loads_kv = [pltpu.make_async_copy(src, wkvbuf.at[:, win(i, LANE)], wkv_sem.at[i]) for i, src in enumerate((wk_ref, wv_ref))]
    for copy in loads_h[:1] + loads_kv + loads_h[1:]:
        copy.start()
    for copy in loads_h[:1] + loads_kv:
        copy.wait()
    for copy in loads_wq:
        copy.start()
    sends = []
    for i, row in enumerate(rows):
        if i:
            loads_h[i].wait()
        kv = dot(hbuf[row, :], wkvbuf[...])
        kvbuf[row, win(0, LANE)] = rope(kv[:, :LANE], cos_ref[...], sin_ref[...])[0].astype(BF16)
        kvbuf[row, win(1, LANE)] = kv[:, LANE:].astype(BF16)
        piece = kv_out.at[cp, row]
        own = pltpu.make_async_copy(kvbuf.at[row], piece, osem.at[2 + i])
        own.start()
        if i == 0:
            pl.semaphore_wait(barrier, len(peers))
        own.wait()
        sends.append([hand_over(piece, piece, send_sem.at[n, i], recv_sem.at[n, i], tp, peer) for n, peer in enumerate(peers)])
        for copy in sends[i]:
            copy.start()
    for copy in loads_wq:
        copy.wait()
    for copy in loads_g + loads_wo:
        copy.start()
    cos2, sin2 = [jnp.concatenate([tab[...]] * 2, axis=0) for tab in (cos_ref, sin_ref)]

    @pl.loop(0, HEADS)
    def _(step):
        row, col = win(lax.div(step, CHIPS), BRICK), win(lax.rem(step, CHIPS), TILE)
        tile = dot(hbuf[row, :], wqbuf[col, :], NT)
        qbuf[row, col] = (jnp.concatenate(rope(tile, cos2, sin2), axis=1) * q_scale).astype(BF16)

    store_q = pltpu.make_async_copy(qbuf, q_out, osem.at[0])
    store_q.start()
    for copy in loads_g + loads_wo:
        copy.wait()
    passes = []

    def pass_on(i):
        for n, peer in enumerate(others):
            sends[i][n].wait_recv()
            piece = kv_out.at[peer, rows[i]]
            copy = hand_over(piece, piece, send_sem.at[CHIPS + n, i], recv_sem.at[CHIPS + n, i], tp, partner)
            copy.start()
            passes.append(copy)

    for half in range(2):
        @pl.loop(half * CHIPS, (half + 1) * CHIPS)
        def _(step):
            row, col = win(lax.div(step, CHIPS), BRICK), win(lax.rem(step, CHIPS), TILE)
            dobuf[row, col] = dot(gbuf[row, :], wobuf[col, :], NT).astype(BF16)

        pass_on(half)
    store_do = pltpu.make_async_copy(dobuf, do_out, osem.at[1])
    store_do.start()
    for i in range(2, CHIPS):
        pass_on(i)
    for group in sends:
        group[-1].wait_recv()
        for copy in group:
            copy.wait_send()
    for copy in passes:
        copy.wait()
    store_q.wait()
    store_do.wait()


def projections(h, g, wq_t, wo2, wk, wv, cos_tab, sin_tab, q_scale):
    square = (ROWS, ROWS)
    kv_shape = (HEADS, ROWS, TILE)
    return pl.pallas_call(
        functools.partial(proj_kernel, q_scale),
        name="projections",
        out_shape=[jax.ShapeDtypeStruct(s, BF16) for s in (square, square, kv_shape)],
        in_specs=[ANY] * 6 + [VM] * 2,
        out_specs=[ANY] * 3,
        scratch_shapes=[pltpu.VMEM(s, BF16) for s in [(ROWS, DEPTH)] * 4 + [(DEPTH, TILE), square, square, (ROWS, TILE)]]
        + [DMA(s) for s in ((CHIPS, CHIPS), (2,), (6,), (7, CHIPS), (7, CHIPS))],
        compiler_params=pltpu.CompilerParams(collective_id=0, has_side_effects=True, vmem_limit_bytes=VMEM_CAP),
        cost_estimate=pl.CostEstimate(flops=20_000_000_000, bytes_accessed=40_000_000, transcendentals=0),
    )(h, g, wq_t, wo2, wk, wv, cos_tab, sin_tab)


def attn_kernel(q_scale, q_ref, do_ref, kv_ref, mask_ref, cos_ref, sin_ref, o_ref, dq_ref, dkv_ref):
    keys = kv_ref[:, :, :LANE].reshape(ROWS, LANE)
    vals = kv_ref[:, :, LANE:].reshape(ROWS, LANE)
    sums = []
    for pair in range(CHIPS):
        cols = [win(2 * pair + i, LANE) for i in range(2)]
        q = jnp.concatenate([q_ref[:, c] for c in cols], axis=0)
        do = jnp.concatenate([do_ref[:, c] for c in cols], axis=0)
        scores = dot(q, keys, NT) + mask_ref[...]
        prob = jnp.exp(scores - jnp.max(scores, axis=1, keepdims=True))
        prob = prob * (1.0 / jnp.sum(prob, axis=1, keepdims=True))
        prob_b = prob.astype(BF16)
        out = dot(prob_b, vals).astype(BF16)
        delta = jnp.sum(do.astype(F32) * out.astype(F32), axis=1, keepdims=True)
        d_score = (prob * (dot(do, vals, NT) - delta)).astype(BF16)
        dq = dot(d_score, keys)
        dq = ((dq * cos_ref[...] - pltpu.roll(dq, LANE // 2, 1) * sin_ref[...]) * q_scale).astype(BF16)
        for i, c in enumerate(cols):
            o_ref[:, c] = out[i * LANE:(i + 1) * LANE]
            dq_ref[:, c] = dq[i * LANE:(i + 1) * LANE]
        sums.append((dot(q.T, d_score), dot(do.T, prob_b)))
    for kind, parts in enumerate(zip(*sums)):
        total = (parts[0] + parts[1]) + (parts[2] + parts[3])
        for j in range(HEADS):
            dkv_ref[j, kind] = total[:, j * LANE:(j + 1) * LANE]


def attention(q, do, kv, mask2, cos_tab, sin_tab, q_scale):
    row_block = pl.BlockSpec((LANE, ROWS), lambda b: (b, 0))
    whole = lambda a: pl.BlockSpec(a.shape, lambda b: (0,) * a.ndim)
    return pl.pallas_call(
        functools.partial(attn_kernel, q_scale),
        name="attention",
        grid=(HEADS,),
        out_shape=[jax.ShapeDtypeStruct((ROWS, ROWS), BF16)] * 2 + [jax.ShapeDtypeStruct((HEADS, 2, TILE, BRICK), F32)],
        in_specs=[row_block, row_block, pl.BlockSpec((HEADS, LANE, TILE), lambda b: (0, b, 0)), whole(mask2), whole(cos_tab), whole(sin_tab)],
        out_specs=[row_block, row_block, pl.BlockSpec((HEADS, 2, LANE, LANE), lambda b: (0, 0, lax.div(b, CHIPS), lax.rem(b, CHIPS)))],
        compiler_params=pltpu.CompilerParams(vmem_limit_bytes=VMEM_CAP),
        cost_estimate=pl.CostEstimate(flops=30_000_000_000, bytes_accessed=20_000_000, transcendentals=8_000_000),
    )(q, do, kv, mask2, cos_tab, sin_tab)


def tables(cp):
    half = LANE // 2
    pos = cp * LANE + jnp.arange(LANE)
    inv_freq = 1.0 / jnp.power(10000.0, jnp.arange(half, dtype=F32) * (2.0 / LANE))
    ang = pos.astype(F32)[:, None] * inv_freq[None, :]
    cos, sin = jnp.cos(ang), jnp.sin(ang)
    double = lambda tab: jnp.tile(tab, (2, 1))
    mask = jnp.where(jnp.arange(ROWS)[None, :] <= pos[:, None], 0.0, -jnp.inf).astype(F32)
    return jnp.concatenate([cos.T, sin.T], axis=0), double(jnp.concatenate([cos, cos], axis=1)), double(jnp.concatenate([-sin, sin], axis=1)), double(mask)


DKV, DWO, DWQ, DWKV = 0, (1, 2), (3, 4), 5
SETS, SLOTS, GROUPS = 6, 5, 8
LEADS, EARLY = (1, 3), 2
FAR_ROLES = (0, 2, 3)
INPUTS = ("o", "dq", "wo", "wq", "near", "mid", "far", "wkv", "g", "h", "dkv", "tabs")
OUTPUTS = {"out": ((ROWS, DEPTH), BF16), "dh": ((ROWS, DEPTH), BF16), "dwo": ((ROWS, DEPTH), F32), "dwq": ((DEPTH, ROWS), F32),
           "dwkv": ((DEPTH, TILE), F32), "dkvb": ((ROWS, TILE), BF16), "wland": ((DEPTH, HALF_W), BF16),
           "pland": ((SETS, CHIPS, BRICK, BRICK), F32), "xland": ((SETS, 2, BRICK, BRICK), F32), "hland": ((SETS, 2, TILE, BRICK), F32), "zland": ((2, BRICK, BRICK), F32)}
BUFFERS = {"abuf": ((ROWS, DEPTH + TILE), BF16), "wa": ((DEPTH + TILE, HALF_W), BF16), "wb": ((DEPTH + TILE, TILE), BF16),
           "tile_a": ((LANE, HALF_W), BF16), "tile_b": ((ROWS, TILE), BF16), "keep": ((SLOTS, CHIPS, BRICK, BRICK), F32),
           "tmp": ((CHIPS, BRICK, BRICK), F32), "stage": ((2, BRICK, BRICK), F32), "left": ((2, ROWS, BRICK), BF16),
           "right": ((2, ROWS, BRICK), BF16), "zbuf": ((BRICK, BRICK), F32)}
SEMS = {"load": (12,), "early": (4,), "asend": (2, GROUPS), "arecv": (2, 3, GROUPS), "wsend": (2, GROUPS), "wrecv": (2, 3, GROUPS), "fsend": (2, 3), "frecv": (2, 3, GROUPS),
        "rsend": (2, 2, 2, GROUPS), "rrecv": (2, 2, GROUPS), "swsend": (3,), "swrecv": (3,), "dsend": (SETS, CHIPS), "drecv": (SETS, CHIPS),
        "xsend": (SETS, 2), "xrecv": (SETS, 2), "hsend": (SETS, 2), "hrecv": (SETS, 2), "zsend": (3,), "zrecv": (3,), "gsend": (SETS, 9), "grecv": (SETS, 9)}


class Exchange:
    def __init__(self, *refs):
        for name, ref in zip((*INPUTS, *OUTPUTS, *BUFFERS, *SEMS, "credit"), refs):
            setattr(self, name, ref)
        self.tp, self.cp = lax.axis_index("tp"), lax.axis_index("cp")
        self.core, self.chip = lax.rem(self.cp, 2), lax.div(self.cp, 2)
        self.x, self.y, self.diag, self.partner = plane_peers(self.cp)
        self.acts, self.weights, self.results = (self.o, self.dq), (self.wo, self.wq), (self.out, self.dh)

    def move(self, pairs):
        copies = [pltpu.make_async_copy(src, dst, self.load.at[i]) for i, (src, dst) in enumerate(pairs)]
        for copy in copies:
            copy.start()
        for copy in copies:
            copy.wait()


    def plane(self, phase, role):
        return CHIPS - 1 - role if phase else role

    def role(self, phase):
        return self.plane(phase, self.tp)

    def act_copy(self, phase, src, i, to):
        row = win(i, LANE)
        return hand_over(self.acts[phase].at[row], self.abuf.at[row, win(src, ROWS)], self.asend.at[phase, i],
                         self.arecv.at[phase, FAR_ROLES.index(src), i], to, self.cp)

    def w_copy(self, phase, src, n, to):
        rows = 2 * src + self.core
        return hand_over(self.weights[phase].at[win(self.core, BRICK), win(GROUPS + n, TILE)], self.wland.at[win(rows, BRICK), win(n, TILE)],
                         self.wsend.at[phase, n], self.wrecv.at[phase, FAR_ROLES.index(src), n], to, self.cp)

    def cross_copy(self, phase, src, n, core):
        place = self.wland.at[win(2 * src + core, BRICK), win(n, TILE)]
        slot = FAR_ROLES.index(src)
        return hand_over(place, place, self.fsend.at[phase, slot], self.frecv.at[phase, slot, n], self.tp, self.partner)

    def piece(self, phase, kind, idx):
        if kind:
            return self.results[phase].at[:, win(GROUPS + idx, TILE)]
        return self.results[phase].at[win(idx, LANE), win(0, HALF_W)]

    def result_copy(self, phase, kind, idx, way, to_role):
        piece = self.piece(phase, kind, idx)
        return hand_over(piece, piece, self.rsend.at[phase, way, kind, idx], self.rrecv.at[phase, kind, idx], self.plane(phase, to_role), self.cp)

    def ask_far(self, phase):
        pl.semaphore_signal(self.credit.at[phase], inc=1, device_id=(self.plane(phase, 3), self.cp), device_id_type=MESH)

    def multiply(self, phase, kind, idx):
        depth = pl.ds(0, DEPTH + TILE * phase)
        act, weight = self.acts[phase], self.weights[phase]
        if kind == 0:
            row = win(idx, LANE)
            for src in FAR_ROLES:
                self.act_copy(phase, src, idx, self.plane(phase, src)).wait_recv()
            self.ask_far(phase)

            @pl.loop(0, CHIPS)
            def _(i):
                col = win(i, BRICK)
                self.tile_a[:, col] = dot(self.abuf[row, depth], self.wa[depth, col]).astype(BF16)
        else:
            for src in FAR_ROLES:
                self.cross_copy(phase, src, idx, 1 - self.core).wait_recv()
                self.cross_copy(phase, src, idx, self.core).wait_send()
            pairs = [(self.wland.at[win(src, ROWS), win(idx, TILE)], self.wb.at[win(src, ROWS)]) for src in FAR_ROLES]
            pairs.append((weight.at[:, win(GROUPS + idx, TILE)], self.wb.at[win(1, ROWS)]))
            if phase:
                pairs.append((self.wkv.at[:, win(GROUPS + idx, TILE)], self.wb.at[pl.ds(DEPTH, TILE)]))
            self.move(pairs)

            @pl.loop(0, CHIPS)
            def _(i):
                row = win(i, TILE)
                self.tile_b[row, :] = dot(self.abuf[row, depth], self.wb[depth, :]).astype(BF16)

        self.move([(self.tile_b if kind else self.tile_a, self.piece(phase, kind, idx))])
        for way, to_role in enumerate((0, 2)):
            self.result_copy(phase, kind, idx, way, to_role).start()

    def swap_weights(self, phase, idx):
        @pl.when(self.role(phase) == 1)
        def _():
            for src in FAR_ROLES:
                self.w_copy(phase, src, idx, self.plane(phase, src)).wait_recv()
                self.cross_copy(phase, src, idx, self.core).start()

            @pl.when(idx < GROUPS - LEADS[phase])
            def _():
                self.ask_far(phase)

    def group(self, phase, kind, idx):
        role = self.role(phase)

        @pl.when(role == 0)
        def _():
            self.result_copy(phase, kind, idx, 0, 1).wait_recv()

        @pl.when(role == 1)
        def _():
            self.multiply(phase, kind, idx)

        @pl.when(role == 2)
        def _():
            self.result_copy(phase, kind, idx, 0, 1).wait_recv()
            self.result_copy(phase, kind, idx, 0, 3).start()

        item = idx + LEADS[phase]

        @pl.when((role == 3) & ((item < GROUPS) | (kind == 0)))
        def _():
            pl.semaphore_wait(self.credit.at[phase], 1)

            @pl.when((item < GROUPS) & (kind == 0))
            def _():
                self.act_copy(phase, 3, item, self.plane(phase, 1)).start()

            @pl.when((item >= GROUPS) | (kind == 1))
            def _():
                self.w_copy(phase, 3, lax.rem(item, GROUPS), self.plane(phase, 1)).start()

    def feed(self, phase, src, acts, weights):
        @pl.when(self.role(phase) == src)
        def _():
            for i in acts:
                self.act_copy(phase, src, i, self.plane(phase, 1)).start()
            for n in weights:
                self.w_copy(phase, src, n, self.plane(phase, 1)).start()

    def start_line(self):
        for phase in range(2):
            @pl.when(self.role(phase) == 1)
            def _():
                swaps = []
                for i, (half, src) in enumerate(zip((self.near, self.mid, self.far), FAR_ROLES)):
                    swaps.append(hand_over(half, self.wa.at[win(2 * src + self.core, BRICK)], self.swsend.at[i], self.swrecv.at[i], self.tp, self.partner))
                    swaps[i].start()
                pairs = [(half, self.wa.at[win(2 * src + self.core, BRICK)]) for half, src in zip((self.near, self.mid, self.far), FAR_ROLES)]
                pairs.append((self.weights[phase].at[:, win(0, HALF_W)], self.wa.at[win(1, ROWS)]))
                pairs.append((self.acts[phase], self.abuf.at[:, win(1, ROWS)]))
                pairs.append((self.wkv.at[:, win(0, HALF_W)], self.wa.at[pl.ds(DEPTH, TILE)]))
                self.move(pairs)

    def end_swap(self):
        @pl.when((self.tp == 1) | (self.tp == 2))
        def _():
            for i, (half, src) in enumerate(zip((self.near, self.mid, self.far), FAR_ROLES)):
                hand_over(half, self.wa.at[win(2 * src + 1 - self.core, BRICK)], self.swsend.at[i], self.swrecv.at[i], self.tp, self.partner).wait()

    def end_line(self):
        for phase in range(2):
            role = self.role(phase)
            for kind in range(2):
                @pl.when(role == 1)
                def _():
                    @pl.loop(0, GROUPS)
                    def _(idx):
                        for way, to_role in enumerate((0, 2)):
                            self.result_copy(phase, kind, idx, way, to_role).wait_send()

                @pl.when(role == 2)
                def _():
                    @pl.loop(0, GROUPS)
                    def _(idx):
                        self.result_copy(phase, kind, idx, 0, 3).wait_send()

                @pl.when(role == 3)
                def _():
                    @pl.loop(0, GROUPS)
                    def _(idx):
                        self.result_copy(phase, kind, idx, 0, 2).wait_recv()

            for src in FAR_ROLES:
                @pl.when(role == src)
                def _():
                    for i in range(GROUPS):
                        self.act_copy(phase, src, i, self.plane(phase, 1)).wait_send()
                        self.w_copy(phase, src, i, self.plane(phase, 1)).wait_send()


    def brick(self, which, ref):
        return ref.at[:, pl.ds(0, TILE)] if which == DWKV else ref

    def pair_copy(self, kind, i, src, which=None):
        which = kind if which is None else which
        return hand_over(src, self.brick(kind, self.pland.at[which, i]), self.dsend.at[which, i], self.drecv.at[which, i], self.tp, self.partner)

    def chip_copies(self, which):
        return [hand_over(self.brick(which, self.keep.at[which % SLOTS, lax.div(peer, 2)]), self.brick(which, self.xland.at[which, n]),
                          self.xsend.at[which, n], self.xrecv.at[which, n], self.tp, peer) for n, peer in enumerate((self.x, self.y))]

    def half_copies(self, which):
        block = self.brick(which, self.keep.at[which % SLOTS, lax.div(self.diag, 2)])
        return [hand_over(block.at[win(n, TILE)], self.brick(which, self.hland.at[which, n]),
                          self.hsend.at[which, n], self.hrecv.at[which, n], self.tp, peer) for n, peer in enumerate((self.x, self.y))]

    def own_blocks(self):
        return [pltpu.make_async_copy(self.dkv.at[2 * i + self.core], self.keep.at[0, i], self.early.at[i]) for i in range(CHIPS)]

    def hand_dkv(self):
        for i in range(CHIPS):
            self.pair_copy(DKV, i, self.dkv.at[2 * i + 1 - self.core]).start()
        for copy in self.own_blocks():
            copy.start()

    def fetch(self, part):
        half, i = win(lax.rem(lax.div(part, CHIPS), 2), BRICK), lax.rem(part, CHIPS)
        narrow = pl.ds(0, TILE)
        for n, block in enumerate((2 * i + 1 - self.core, 2 * i + self.core)):
            block = win(block, BRICK)
            right = self.right.at[n]
            for kind, pair in enumerate((((self.o.at[:, half], self.left.at[n]), (self.g.at[:, block], right)),
                                         ((self.h.at[:, block], self.left.at[n]), (self.dq.at[:, half], right)),
                                         ((self.h.at[:, block], self.left.at[n]), (self.dkvb, right.at[:, narrow])))):
                @pl.when(lax.div(part, 2 * CHIPS) == kind)
                def _():
                    for m, (src, dst) in enumerate(pair):
                        pltpu.make_async_copy(src, dst, self.early.at[2 * n + m]).start()

    def make(self, part, which=None):
        kind, i = which, lax.rem(part, CHIPS)
        which = 1 + lax.div(part, CHIPS) if which is None else which
        col = pl.ds(0, BRICK if kind is None else TILE)
        slot = self.stage.at[lax.rem(part, 2), :, col]

        @pl.when(i > 1)
        def _():
            self.pair_copy(kind, i - 2, slot, which).wait_send()

        for n, dst in enumerate((slot, self.keep.at[lax.rem(which, SLOTS), i, :, col])):
            left, right = self.left.at[n], self.right.at[n, :, col]
            for m, factor in enumerate((left, right)):
                pltpu.make_async_copy(self.h.at[:, col] if m else self.h.at[:, win(0, BRICK)], factor, self.early.at[2 * n + m]).wait()
            dst[...] = dot(left[...], right[...], TN)
            if n == 0:
                self.pair_copy(kind, i, slot, which).start()

        @pl.when((part != PARTS - 1) & (part != PARTS + CHIPS - 1))
        def _():
            self.fetch(part + 1)

    def total(self, which, count, add):
        @pl.loop(0, count * HEADS)
        def _(step):
            add(lax.div(step, HEADS), win(lax.rem(step, HEADS), LANE // 2))

    def add_pair(self, which):
        keep = self.keep.at[which % SLOTS]
        landed = [self.brick(which, self.pland.at[which, i]) for i in range(CHIPS)]
        for i in range(CHIPS):
            self.pair_copy(which, i, landed[i]).wait_recv()
        for i in range(0 if which == DKV else CHIPS // 2, CHIPS):
            self.pair_copy(which, i, landed[i]).wait_send()
        if which == DKV:
            for copy in self.own_blocks():
                copy.wait()
            self.fetch(0)
        self.move([(landed[i], self.brick(which, self.tmp.at[i])) for i in range(CHIPS)])
        col = pl.ds(0, TILE if which == DWKV else BRICK)

        def add(i, row):
            keep[i, row, col] = keep[i, row, col] + self.tmp[i, row, col]

        self.total(which, CHIPS, add)
        for copy in self.half_copies(which):
            copy.start()

    def relay(self, which):
        for copy in self.half_copies(which):
            copy.wait()
        self.move([(self.brick(which, self.hland.at[which, n]), self.brick(which, self.tmp.at[n, win(0, TILE)])) for n in range(2)])
        col = pl.ds(0, TILE if which == DWKV else BRICK)
        for n, peer in enumerate((self.y, self.x)):
            block = self.keep.at[which % SLOTS, lax.div(peer, 2)]
            for step in range(CHIPS):
                row, src = win(CHIPS * n + step, LANE // 2), win(step, LANE // 2)
                block[row, col] = block[row, col] + self.tmp[n, src, col]
        for copy in self.chip_copies(which):
            copy.start()

    def place(self, which, owner):
        if which in DWO:
            return self.dwo.at[win(which - DWO[0], BRICK), win(owner, BRICK)]
        if which in DWQ:
            return self.dwq.at[win(owner, BRICK), win(which - DWQ[0], BRICK)]
        return self.dwkv.at[win(owner, BRICK)]

    def share_copy(self, which, kind):
        owner = (self.cp, self.cp, self.cp, self.x, self.y, self.y, self.x, self.diag, self.diag)[kind]
        to = (self.x, self.y, self.partner, self.partner, self.partner, self.x, self.y, self.partner, self.partner)[kind]
        place = self.place(which, owner)
        if kind > 4:
            place = place.at[win((kind + 1) % 2, TILE)]
        return hand_over(place, place, self.gsend.at[which, kind], self.grecv.at[which, kind], self.tp, to)

    def shared_place(self, which, kind):
        mate = lambda idx: plane_peers(idx)[-1]
        owner = (self.x, self.y, self.partner, mate(self.x), mate(self.y), self.diag, self.diag, mate(self.diag), mate(self.diag))[kind]
        place = self.place(which, owner)
        if kind > 4:
            place = place.at[win((kind + 1) % 2, TILE)]
        return hand_over(place, place, self.gsend.at[which, kind], self.grecv.at[which, kind], self.tp, self.partner)

    def add_chips(self, which):
        copies = self.chip_copies(which)
        for copy in copies:
            copy.wait()
        self.move([(self.brick(which, self.xland.at[which, n]), self.brick(which, self.tmp.at[n])) for n in range(len(copies))])
        col = pl.ds(0, TILE if which == DWKV else BRICK)
        own = self.keep.at[which % SLOTS, self.chip]

        def add(_, row):
            own[row, col] = own[row, col] + (self.tmp[0, row, col] + self.tmp[1, row, col])

        self.total(which, 1, add)
        if which == DKV:
            self.total(which, 1, self.keep_z)
            for end, inner in ((0, 1), (3, 2)):
                @pl.when(self.tp == end)
                def _():
                    self.z_copy(0, inner).start()
            return
        self.move([(self.brick(which, own), self.place(which, self.cp))])
        for kind in range(3):
            self.share_copy(which, kind).start()

    def pass_on(self, which):
        for kind in range(2):
            self.shared_place(which, kind).wait_recv()
        for kind in (5, 6, 3, 4):
            self.share_copy(which, kind).start()

    def pass_diagonal(self, which):
        for kind in (5, 6):
            self.shared_place(which, kind).wait_recv()
        for kind in (7, 8):
            self.share_copy(which, kind).start()

    def end_share(self, which):
        for kind in (2, 3, 4, 7, 8):
            self.shared_place(which, kind).wait_recv()
        for kind in range(9):
            self.share_copy(which, kind).wait_send()


    def keep_z(self, _, row):
        self.zbuf[row] = self.keep[0, self.chip, row]

    def z_copy(self, slot, to):
        return hand_over(self.zbuf, self.zland.at[slot], self.zsend.at[slot], self.zrecv.at[slot], to, self.cp)

    def z_result(self, slot, to):
        return hand_over(self.dkvb, self.dkvb, self.zsend.at[slot], self.zrecv.at[2], to, self.cp)

    def meet(self):
        for inner in (1, 2):
            @pl.when(self.tp == inner)
            def _():
                self.z_copy(0, CHIPS - 1 - inner).wait_recv()
                self.move([(self.zland.at[0], self.tmp.at[0])])

                def add(_, row):
                    self.zbuf[row] = self.zbuf[row] + self.tmp[0, row]

                self.total(DKV, 1, add)
                if inner == 2:
                    self.z_copy(1, 1).start()

    def settle(self):
        half = LANE // 2

        @pl.when(self.tp == 1)
        def _():
            self.z_copy(1, 2).wait_recv()
            self.move([(self.zland.at[1], self.tmp.at[0]), (self.tabs, self.tmp.at[1, win(0, LANE), win(0, LANE)])])
            for b in range(HEADS):
                cos, sin = self.tmp[1, win(0, half), win(0, LANE)], self.tmp[1, win(1, half), win(0, LANE)]
                for kind in range(2):
                    row, col = win(2 * kind + b // CHIPS, LANE), win(b % CHIPS, LANE)
                    part = self.zbuf[row, col] + self.tmp[0, row, col]
                    if kind == 0:
                        low, high = part[:half], part[half:]
                        part = jnp.concatenate([low * cos + high * sin, high * cos - low * sin], axis=0)
                    self.abuf[win(b, LANE), win(DEPTH // LANE + kind, LANE)] = part.T.astype(BF16)
            self.move([(self.abuf.at[:, pl.ds(DEPTH, TILE)], self.dkvb)])
            self.z_result(2, 2).start()
            self.z_result(0, 0).start()

    def take(self):
        @pl.when(self.tp == 2)
        def _():
            self.z_result(2, 1).wait_recv()
            self.z_result(2, 3).start()
            self.move([(self.dkvb, self.abuf.at[:, pl.ds(DEPTH, TILE)])])

    def get_result(self):
        for end in (0, 3):
            @pl.when(self.tp == end)
            def _():
                self.z_result(2, 1).wait_recv()
                self.z_copy(0, 1).wait_send()

        @pl.when(self.tp == 1)
        def _():
            self.z_result(0, 0).wait_send()

        @pl.when(self.tp == 2)
        def _():
            self.z_copy(1, 1).wait_send()

        @pl.when((self.tp == 1) | (self.tp == 2))
        def _():
            self.z_result(2, 3).wait_send()

        self.fetch(PARTS)


STEPS = {"add_pair": ((1, 3, 5, 7, 9, 22), (1, 5, 9, 13, 17, 23)), "relay": ((3, 6, 7, 10, 13, 24), (4, 8, 12, 16, 20, 25)),
         "add_chips": ((6, 10, 13, 15, 18, 26), (7, 11, 15, 19, 23, 28)), "pass_on": ((0, 25, 26, 27, 28, 29), (0, 15, 19, 23, 27, 30)),
         "pass_diagonal": ((0, 28, 29, 30, 31, 31), (0, 19, 23, 27, 31, 31))}
ONCE = {"hand_dkv": 0, "meet": 10, "settle": 15, "get_result": 17}
PARTS, LATE = 16, 18


def exchange_kernel(*refs):
    dev = Exchange(*refs)
    barrier = pltpu.get_barrier_semaphore()
    for step in range(1, CHIPS):
        pl.semaphore_signal(barrier, inc=1, device_id=(lax.rem(dev.tp + step, CHIPS), dev.cp), device_id_type=MESH)
    for peer in plane_peers(dev.cp):
        pl.semaphore_signal(barrier, inc=1, device_id=(dev.tp, peer), device_id_type=MESH)
    pl.semaphore_wait(barrier, 7)
    blocks = range(GROUPS)
    dev.feed(0, 3, blocks[:LEADS[0]], ())
    dev.feed(0, 0, blocks[:1], ())
    for i in blocks[1:]:
        dev.feed(0, 0, (i,), ())
        if i <= LEADS[1]:
            dev.feed(1, 3, (i - 1,), ())
    dev.feed(0, 0, (), blocks)
    dev.feed(0, 2, blocks, blocks)
    dev.feed(1, 2, blocks[:EARLY], ())
    dev.start_line()
    dev.end_swap()
    busy = dev.tp == 2

    @pl.loop(0, CHIPS * GROUPS)
    def _(now):
        idx = lax.rem(now, GROUPS)
        spans = [(lax.div(now, GROUPS) == 2 * phase + kind, phase, kind) for phase in range(2) for kind in range(2)]

        @pl.when(now == 2 * GROUPS)
        def _():
            dev.feed(1, 0, blocks, blocks)
            dev.feed(1, 2, blocks[EARLY:], blocks)
            dev.take()

        for here, phase, kind in spans:
            @pl.when(here)
            def _():
                if kind:
                    dev.swap_weights(phase, idx)
                else:
                    dev.group(phase, kind, idx)

        for step, at in ONCE.items():
            @pl.when(now == at)
            def _():
                getattr(dev, step)()

        for step, (early, late) in STEPS.items():
            for which in range(SETS):
                if late[which]:
                    @pl.when(now == jnp.where(busy, early[which], late[which]))
                    def _():
                        getattr(dev, step)(which)

        @pl.loop(jnp.where(busy, jnp.maximum(2 * now - 2, 0), jnp.maximum(now - 1, 0)), jnp.minimum(jnp.where(busy, 2 * now, now), PARTS))
        def _(part):
            dev.make(part)

        @pl.when((now >= LATE) & (now < LATE + CHIPS))
        def _():
            dev.make(now + PARTS - LATE, DWKV)

        for here, phase, kind in spans:
            if kind:
                @pl.when(here)
                def _():
                    dev.group(phase, kind, idx)

    for which in range(1, SETS):
        dev.end_share(which)
    dev.end_line()


def exchange(*operands):
    return pl.pallas_call(
        exchange_kernel,
        name="exchange",
        out_shape=[jax.ShapeDtypeStruct(*spec) for spec in OUTPUTS.values()],
        in_specs=[ANY] * len(operands),
        out_specs=[ANY] * len(OUTPUTS),
        scratch_shapes=[pltpu.VMEM(*spec) for spec in BUFFERS.values()] + [DMA(shape) for shape in SEMS.values()] + [pltpu.SemaphoreType.REGULAR((2,))],
        compiler_params=pltpu.CompilerParams(collective_id=1, has_side_effects=True, vmem_limit_bytes=VMEM_CAP),
        cost_estimate=pl.CostEstimate(flops=300_000_000_000, bytes_accessed=200_000_000, transcendentals=0),
    )(*operands)


def solution(mesh):
    def local_program(hidden, grad_out, w_query, w_key, w_value, w_out):
        tp, cp = lax.axis_index("tp"), lax.axis_index("cp")
        h, g = hidden.reshape(ROWS, DEPTH), grad_out.reshape(ROWS, DEPTH)
        q_scale = LANE ** -0.5
        tabs, cos_tab, sin_tab, mask2 = tables(cp)
        wo2 = w_out.reshape(ROWS, DEPTH)
        wq_t = w_query.transpose(1, 2, 0).reshape(ROWS, DEPTH)
        wkv_t = jnp.concatenate([w_key, w_value], axis=1).T
        wo_half, wq_half = [lax.dynamic_slice(w, (lax.rem(cp, 2) * BRICK, 0), (BRICK, HALF_W)) for w in (wo2, wq_t)]
        one_way, other_way = jnp.where(tp <= 1, wo_half, wq_half), jnp.where(tp <= 1, wq_half, wo_half)
        near = lax.ppermute(one_way, "tp", [(0, 1), (3, 2)])
        mid = lax.ppermute(other_way, "tp", [(2, 1), (1, 2)])
        far = lax.ppermute(other_way, "tp", [(3, 1), (0, 2)])
        q, d_o, kv = projections(h, g, wq_t, wo2, w_key, w_value, cos_tab, sin_tab, q_scale)
        o, dq, dkv = attention(q, d_o, kv, mask2, cos_tab, sin_tab, q_scale)
        out, dh, dwo, dwq, dwkv = exchange(o, dq, wo2, wq_t, near, mid, far, wkv_t, g, h, dkv.reshape(HEADS, BRICK, BRICK), tabs)[:5]
        return (out.reshape(hidden.shape), dh.reshape(hidden.shape), dwq.reshape(w_query.shape),
                dwkv[:, :LANE], dwkv[:, LANE:], dwo.reshape(w_out.shape))

    row_spec, head_spec = P(None, "cp", None), P("tp", None, None)
    query_spec = P(None, "tp", None)
    return jax.shard_map(local_program, mesh=mesh, in_specs=(row_spec, row_spec, query_spec, P(), P(), head_spec),
                         out_specs=(row_spec, row_spec, query_spec, P(), P(), head_spec), check_vma=False)
```

```python
import functools
import jax
import jax.numpy as jnp
from jax import lax
from jax.experimental import pallas as pl
from jax.experimental.pallas import tpu as pltpu
from jax.sharding import PartitionSpec as P

ROWS, DEPTH, LANE, TILE, BRICK, HALF_W = 1024, 4096, 128, 256, 512, 2048
CHIPS, HEADS, GROUPS = 4, 8, 8
VMEM_CAP = 66_000_000
MESH = pl.DeviceIdType.MESH
F32, BF16 = jnp.float32, jnp.bfloat16
NT = (((1,), (1,)), ((), ()))
NN = (((1,), (0,)), ((), ()))
TN = (((0,), (0,)), ((), ()))
ANY = pl.BlockSpec(memory_space=pl.ANY)
VM = pl.BlockSpec(memory_space=pltpu.VMEM)
DMA = pltpu.SemaphoreType.DMA


def dot(lhs, rhs, dims=NN):
    return lax.dot_general(lhs, rhs, dims, preferred_element_type=F32)


def cost(gigaflops):
    return pl.CostEstimate(flops=gigaflops * 10 ** 9, bytes_accessed=10 ** 8, transcendentals=0)


def talking(collective_id):
    return pltpu.CompilerParams(collective_id=collective_id, has_side_effects=True, vmem_limit_bytes=VMEM_CAP)


def by_row(reduce, tile):
    return reduce(tile, axis=1, keepdims=True)


def twice(tile):
    return jnp.concatenate([tile, tile], axis=0)


def win(index, size):
    start = index * size
    return pl.ds(start if isinstance(start, int) else pl.multiple_of(start, size), size)


def plane_peers(cp):
    x_of = lambda idx: idx + 2 - CHIPS * lax.rem(lax.div(idx, 2), 2)
    y_of = lambda idx: lax.rem(idx + CHIPS, HEADS)
    return x_of(cp), y_of(cp), x_of(y_of(cp)), cp + 1 - 2 * lax.rem(cp, 2)


def hand_over(src, dst, send_sem, recv_sem, tp, cp):
    return pltpu.make_async_remote_copy(src, dst, send_sem, recv_sem, device_id=(tp, cp), device_id_type=MESH)


def rope(tile, cos, sin):
    heads = [tile[:, lo:lo + LANE] for lo in range(0, tile.shape[1], LANE)]
    return [one * cos + pltpu.roll(one, LANE // 2, 1) * sin for one in heads]


def proj_kernel(q_scale, h_ref, g_ref, wq_ref, wo_ref, wk_ref, wv_ref, cos_ref, sin_ref,
                q_out, do_out, kv_out, hbuf, gbuf, wqbuf, wobuf, wkvbuf, qbuf, dobuf, kvbuf,
                load_sem, wkv_sem, osem, send_sem, recv_sem):
    tp, cp = lax.axis_index("tp"), lax.axis_index("cp")
    peers = plane_peers(cp)
    *others, partner = peers
    barrier = pltpu.get_barrier_semaphore()
    for peer in peers:
        pl.semaphore_signal(barrier, inc=1, device_id=(tp, peer), device_id_type=MESH)
    rows = [win(i, TILE) for i in range(CHIPS)]
    loads_h, loads_g, loads_wq, loads_wo = [
        [pltpu.make_async_copy(src.at[r], dst.at[r], load_sem.at[which, i]) for i, r in enumerate(rows)]
        for which, (src, dst) in enumerate(((h_ref, hbuf), (g_ref, gbuf), (wq_ref, wqbuf), (wo_ref, wobuf)))]
    loads_kv = [pltpu.make_async_copy(src, wkvbuf.at[:, win(i, LANE)], wkv_sem.at[i]) for i, src in enumerate((wk_ref, wv_ref))]
    for copy in loads_h[:1] + loads_kv + loads_h[1:]:
        copy.start()
    for copy in loads_h[:1] + loads_kv:
        copy.wait()
    for copy in loads_wq:
        copy.start()
    cos, sin = twice(cos_ref[...]), twice(sin_ref[...])
    sends, stored = [], []

    def share(i):
        piece = kv_out.at[cp, rows[i]]
        stored[i].wait()
        sends.append([hand_over(piece, piece, send_sem.at[n, i], recv_sem.at[n, i], tp, peer) for n, peer in enumerate(peers)])
        for copy in sends[i]:
            copy.start()

    for i, row in enumerate(rows):
        if i:
            loads_h[i].wait()
        kv = dot(hbuf[row, :], wkvbuf[...])
        kvbuf[row, win(0, LANE)] = rope(kv[:, :LANE], cos, sin)[0].astype(BF16)
        kvbuf[row, win(1, LANE)] = kv[:, LANE:].astype(BF16)
        stored.append(pltpu.make_async_copy(kvbuf.at[row], kv_out.at[cp, row], osem.at[2 + i]))
        stored[i].start()
        if i == 0:
            pl.semaphore_wait(barrier, len(peers))
        else:
            share(i - 1)
    share(CHIPS - 1)
    for copy in loads_wq:
        copy.wait()
    for copy in loads_g + loads_wo:
        copy.start()
    cos2, sin2 = twice(cos), twice(sin)

    @pl.loop(0, HEADS)
    def _(step):
        row, col = win(lax.div(step, CHIPS), BRICK), win(lax.rem(step, CHIPS), TILE)
        tile = dot(hbuf[row, :], wqbuf[col, :], NT)
        qbuf[row, col] = (jnp.concatenate(rope(tile, cos2, sin2), axis=1) * q_scale).astype(BF16)

    store_q = pltpu.make_async_copy(qbuf, q_out, osem.at[0])
    store_q.start()
    for copy in loads_g + loads_wo:
        copy.wait()
    passes = []

    def pass_on(i):
        for n, peer in enumerate(others):
            sends[i][n].wait_recv()
            piece = kv_out.at[peer, rows[i]]
            copy = hand_over(piece, piece, send_sem.at[CHIPS + n, i], recv_sem.at[CHIPS + n, i], tp, partner)
            copy.start()
            passes.append(copy)

    for half in range(2):
        @pl.loop(half * CHIPS, (half + 1) * CHIPS)
        def _(step):
            row, col = win(lax.div(step, CHIPS), BRICK), win(lax.rem(step, CHIPS), TILE)
            dobuf[row, col] = dot(gbuf[row, :], wobuf[col, :], NT).astype(BF16)

        pass_on(half)
    store_do = pltpu.make_async_copy(dobuf, do_out, osem.at[1])
    store_do.start()
    for i in range(2, CHIPS):
        pass_on(i)
    for group in sends:
        group[-1].wait_recv()
        for copy in group:
            copy.wait_send()
    for copy in passes:
        copy.wait()
    store_q.wait()
    store_do.wait()


def turn_kernel(w_ref, out_ref):
    out_ref[...] = w_ref[...].reshape(BRICK, ROWS).T


def turn(w):
    return pl.pallas_call(
        turn_kernel,
        name="turn",
        grid=(GROUPS,),
        out_shape=jax.ShapeDtypeStruct((ROWS, DEPTH), BF16),
        in_specs=[pl.BlockSpec((BRICK, HEADS, LANE), lambda i: (i, 0, 0))],
        out_specs=pl.BlockSpec((ROWS, BRICK), lambda i: (0, i)),
        compiler_params=pltpu.CompilerParams(vmem_limit_bytes=VMEM_CAP),
        cost_estimate=cost(1),
    )(w)


def projections(h, g, wq_t, wo2, wk, wv, cos_tab, sin_tab, q_scale):
    square = (ROWS, ROWS)
    kv_shape = (HEADS, ROWS, TILE)
    return pl.pallas_call(
        functools.partial(proj_kernel, q_scale),
        name="projections",
        out_shape=[jax.ShapeDtypeStruct(s, BF16) for s in (square, square, kv_shape)],
        in_specs=[ANY] * 6 + [VM] * 2,
        out_specs=[ANY] * 3,
        scratch_shapes=[pltpu.VMEM(s, BF16) for s in [(ROWS, DEPTH)] * 4 + [(DEPTH, TILE), square, square, (ROWS, TILE)]]
        + [DMA(s) for s in ((CHIPS, CHIPS), (2,), (6,), (7, CHIPS), (7, CHIPS))],
        compiler_params=talking(0),
        cost_estimate=cost(20),
    )(h, g, wq_t, wo2, wk, wv, cos_tab, sin_tab)


def attn_kernel(q_scale, q_ref, do_ref, kv_ref, mask_ref, cos_ref, sin_ref, o_ref, dq_ref, dkv_ref):
    keys = kv_ref[:, :, :LANE].reshape(ROWS, LANE)
    vals = kv_ref[:, :, LANE:].reshape(ROWS, LANE)
    cos, sin, mask = twice(cos_ref[...]), twice(sin_ref[...]), twice(mask_ref[...])
    sums = []
    for pair in range(CHIPS):
        cols = [win(2 * pair + i, LANE) for i in range(2)]
        q = jnp.concatenate([q_ref[:, c] for c in cols], axis=0)
        do = jnp.concatenate([do_ref[:, c] for c in cols], axis=0)
        scores = dot(q, keys, NT) + mask
        prob = jnp.exp(scores - by_row(jnp.max, scores))
        prob = prob * (1.0 / by_row(jnp.sum, prob))
        prob_b = prob.astype(BF16)
        out = dot(prob_b, vals).astype(BF16)
        delta = by_row(jnp.sum, do.astype(F32) * out.astype(F32))
        d_score = (prob * (dot(do, vals, NT) - delta)).astype(BF16)
        dq = dot(d_score, keys)
        dq = ((dq * cos - pltpu.roll(dq, LANE // 2, 1) * sin) * q_scale).astype(BF16)
        for i, c in enumerate(cols):
            o_ref[:, c] = out[i * LANE:(i + 1) * LANE]
            dq_ref[:, c] = dq[i * LANE:(i + 1) * LANE]
        sums.append((dot(q.T, d_score), dot(do.T, prob_b)))
    for kind, parts in enumerate(zip(*sums)):
        total = (parts[0] + parts[1]) + (parts[2] + parts[3])
        for j in range(HEADS):
            dkv_ref[j, kind] = total[:, j * LANE:(j + 1) * LANE]


def attention(q, do, kv, mask, cos_tab, sin_tab, q_scale):
    row_block = pl.BlockSpec((LANE, ROWS), lambda b: (b, 0))
    whole = lambda a: pl.BlockSpec(a.shape, lambda b: (0,) * a.ndim)
    return pl.pallas_call(
        functools.partial(attn_kernel, q_scale),
        name="attention",
        grid=(HEADS,),
        out_shape=[jax.ShapeDtypeStruct((ROWS, ROWS), BF16)] * 2 + [jax.ShapeDtypeStruct((HEADS, 2, TILE, BRICK), F32)],
        in_specs=[row_block, row_block, pl.BlockSpec((HEADS, LANE, TILE), lambda b: (0, b, 0)), whole(mask), whole(cos_tab), whole(sin_tab)],
        out_specs=[row_block, row_block, pl.BlockSpec((HEADS, 2, LANE, LANE), lambda b: (0, 0, lax.div(b, CHIPS), lax.rem(b, CHIPS)))],
        compiler_params=pltpu.CompilerParams(vmem_limit_bytes=VMEM_CAP),
        cost_estimate=cost(30),
    )(q, do, kv, mask, cos_tab, sin_tab)


def tables(cp):
    half = LANE // 2
    pos = cp * LANE + jnp.arange(LANE)
    inv_freq = 1.0 / jnp.power(10000.0, jnp.arange(half, dtype=F32) * (2.0 / LANE))
    ang = pos.astype(F32)[:, None] * inv_freq[None, :]
    cos, sin = jnp.cos(ang), jnp.sin(ang)
    mask = jnp.where(jnp.arange(ROWS)[None, :] <= pos[:, None], 0.0, -jnp.inf).astype(F32)
    return jnp.concatenate([cos.T, sin.T], axis=0), jnp.concatenate([cos, cos], axis=1), jnp.concatenate([-sin, sin], axis=1), mask


DKV, DWO, DWQ, DWKV = 0, (1, 2), (3, 4), 5
SETS, SLOTS = 6, 5
LEADS, EARLY = (1, 3), 2
FAR_ROLES = (0, 2, 3)
INPUTS = ("o", "dq", "wo", "wq", "near", "mid", "far", "wk", "wv", "g", "h", "dkv", "tabs")
OUTPUTS = {"out": ((ROWS, DEPTH), BF16), "dh": ((ROWS, DEPTH), BF16), "dwo": ((ROWS, DEPTH), F32), "dwq": ((DEPTH, ROWS), F32),
           "dwkv": ((DEPTH, TILE), F32), "dkvb": ((ROWS, TILE), BF16), "wland": ((DEPTH, HALF_W), BF16),
           "pland": ((SETS, CHIPS, BRICK, BRICK), F32), "xland": ((SETS, 2, BRICK, BRICK), F32), "hland": ((SETS, 2, TILE, BRICK), F32), "zland": ((2, BRICK, BRICK), F32)}
BUFFERS = {"abuf": ((ROWS, DEPTH + TILE), BF16), "wa": ((DEPTH, HALF_W), BF16), "wb": ((DEPTH, TILE), BF16), "wkv": ((DEPTH, TILE), BF16),
           "tile_a": ((LANE, HALF_W), BF16), "tile_b": ((ROWS, TILE), BF16), "keep": ((SLOTS, CHIPS, BRICK, BRICK), F32),
           "tmp": ((CHIPS, BRICK, BRICK), F32), "stage": ((2, BRICK, BRICK), F32), "left": ((2, ROWS, BRICK), BF16),
           "right": ((2, ROWS, BRICK), BF16), "zbuf": ((BRICK, BRICK), F32)}
SEMS = {"load": (12,), "early": (4,), "asend": (2, GROUPS), "arecv": (2, 3, GROUPS), "wsend": (2, GROUPS), "wrecv": (2, 3, GROUPS), "fsend": (2, 3), "frecv": (2, 3, GROUPS),
        "rsend": (2, 2, 2, GROUPS), "rrecv": (2, 2, GROUPS), "swsend": (3,), "swrecv": (3,), "dsend": (SETS, CHIPS), "drecv": (SETS, CHIPS),
        "xsend": (SETS, 2), "xrecv": (SETS, 2), "hsend": (SETS, 2), "hrecv": (SETS, 2), "zsend": (3,), "zrecv": (3,), "gsend": (SETS, 9), "grecv": (SETS, 9)}


class Exchange:
    def __init__(self, *refs):
        for name, ref in zip((*INPUTS, *OUTPUTS, *BUFFERS, *SEMS, "credit"), refs):
            setattr(self, name, ref)
        self.tp, self.cp = lax.axis_index("tp"), lax.axis_index("cp")
        self.core, self.chip = lax.rem(self.cp, 2), lax.div(self.cp, 2)
        self.x, self.y, self.diag, self.partner = plane_peers(self.cp)
        self.acts, self.weights, self.results = (self.o, self.dq), (self.wo, self.wq), (self.out, self.dh)

    def move(self, pairs):
        copies = [pltpu.make_async_copy(src, dst, self.load.at[i]) for i, (src, dst) in enumerate(pairs)]
        for copy in copies:
            copy.start()
        for copy in copies:
            copy.wait()


    def plane(self, phase, role):
        return CHIPS - 1 - role if phase else role

    def role(self, phase):
        return self.plane(phase, self.tp)

    def act_copy(self, phase, src, i, to):
        row = win(i, LANE)
        return hand_over(self.acts[phase].at[row], self.abuf.at[row, win(src, ROWS)], self.asend.at[phase, i],
                         self.arecv.at[phase, FAR_ROLES.index(src), i], to, self.cp)

    def w_copy(self, phase, src, n, to):
        rows = 2 * src + self.core
        return hand_over(self.weights[phase].at[win(self.core, BRICK), win(GROUPS + n, TILE)], self.wland.at[win(rows, BRICK), win(n, TILE)],
                         self.wsend.at[phase, n], self.wrecv.at[phase, FAR_ROLES.index(src), n], to, self.cp)

    def cross_copy(self, phase, src, n, core):
        place = self.wland.at[win(2 * src + core, BRICK), win(n, TILE)]
        slot = FAR_ROLES.index(src)
        return hand_over(place, place, self.fsend.at[phase, slot], self.frecv.at[phase, slot, n], self.tp, self.partner)

    def piece(self, phase, kind, idx):
        if kind:
            return self.results[phase].at[:, win(GROUPS + idx, TILE)]
        return self.results[phase].at[win(idx, LANE), win(0, HALF_W)]

    def result_copy(self, phase, kind, idx, way, to_role):
        piece = self.piece(phase, kind, idx)
        return hand_over(piece, piece, self.rsend.at[phase, way, kind, idx], self.rrecv.at[phase, kind, idx], self.plane(phase, to_role), self.cp)

    def ask_far(self, phase):
        pl.semaphore_signal(self.credit.at[phase], inc=1, device_id=(self.plane(phase, 3), self.cp), device_id_type=MESH)

    def multiply(self, phase, kind, idx):
        weight = self.weights[phase]

        def product(row, weights, col):
            total = dot(self.abuf[row, pl.ds(0, DEPTH)], weights)
            if phase:
                total = total + dot(self.abuf[row, pl.ds(DEPTH, TILE)], self.wkv[col, :], NT)
            return total.astype(BF16)

        if kind == 0:
            row = win(idx, LANE)
            for src in FAR_ROLES:
                self.act_copy(phase, src, idx, self.plane(phase, src)).wait_recv()
            self.ask_far(phase)

            @pl.loop(0, CHIPS)
            def _(i):
                col = win(i, BRICK)
                self.tile_a[:, col] = product(row, self.wa[:, col], col)
        else:
            for src in FAR_ROLES:
                self.cross_copy(phase, src, idx, 1 - self.core).wait_recv()
                self.cross_copy(phase, src, idx, self.core).wait_send()
            pairs = [(self.wland.at[win(src, ROWS), win(idx, TILE)], self.wb.at[win(src, ROWS)]) for src in FAR_ROLES]
            pairs.append((weight.at[:, win(GROUPS + idx, TILE)], self.wb.at[win(1, ROWS)]))
            self.move(pairs)

            @pl.loop(0, CHIPS)
            def _(i):
                row = win(i, TILE)
                self.tile_b[row, :] = product(row, self.wb[...], win(GROUPS + idx, TILE))

        self.move([(self.tile_b if kind else self.tile_a, self.piece(phase, kind, idx))])
        for way, to_role in enumerate((0, 2)):
            self.result_copy(phase, kind, idx, way, to_role).start()

    def swap_weights(self, phase, idx):
        @pl.when(self.role(phase) == 1)
        def _():
            for src in FAR_ROLES:
                self.w_copy(phase, src, idx, self.plane(phase, src)).wait_recv()
                self.cross_copy(phase, src, idx, self.core).start()

            @pl.when(idx < GROUPS - LEADS[phase])
            def _():
                self.ask_far(phase)

    def group(self, phase, kind, idx):
        role = self.role(phase)

        @pl.when(role == 0)
        def _():
            self.result_copy(phase, kind, idx, 0, 1).wait_recv()

        @pl.when(role == 1)
        def _():
            self.multiply(phase, kind, idx)

        @pl.when(role == 2)
        def _():
            self.result_copy(phase, kind, idx, 0, 1).wait_recv()
            self.result_copy(phase, kind, idx, 0, 3).start()

        item = idx + LEADS[phase]

        @pl.when((role == 3) & ((item < GROUPS) | (kind == 0)))
        def _():
            pl.semaphore_wait(self.credit.at[phase], 1)

            @pl.when((item < GROUPS) & (kind == 0))
            def _():
                self.act_copy(phase, 3, item, self.plane(phase, 1)).start()

            @pl.when((item >= GROUPS) | (kind == 1))
            def _():
                self.w_copy(phase, 3, lax.rem(item, GROUPS), self.plane(phase, 1)).start()

    def feed(self, phase, src, acts, weights):
        @pl.when(self.role(phase) == src)
        def _():
            for i in acts:
                self.act_copy(phase, src, i, self.plane(phase, 1)).start()
            for n in weights:
                self.w_copy(phase, src, n, self.plane(phase, 1)).start()

    def start_line(self):
        for phase in range(2):
            @pl.when(self.role(phase) == 1)
            def _():
                swaps = []
                for i, (half, src) in enumerate(zip((self.near, self.mid, self.far), FAR_ROLES)):
                    swaps.append(hand_over(half, self.wa.at[win(2 * src + self.core, BRICK)], self.swsend.at[i], self.swrecv.at[i], self.tp, self.partner))
                    swaps[i].start()
                pairs = [(half, self.wa.at[win(2 * src + self.core, BRICK)]) for half, src in zip((self.near, self.mid, self.far), FAR_ROLES)]
                pairs.append((self.weights[phase].at[:, win(0, HALF_W)], self.wa.at[win(1, ROWS)]))
                pairs.append((self.acts[phase], self.abuf.at[:, win(1, ROWS)]))
                pairs += [(src, self.wkv.at[:, win(i, LANE)]) for i, src in enumerate((self.wk, self.wv))]
                self.move(pairs)

    def end_swap(self):
        @pl.when((self.tp == 1) | (self.tp == 2))
        def _():
            for i, (half, src) in enumerate(zip((self.near, self.mid, self.far), FAR_ROLES)):
                hand_over(half, self.wa.at[win(2 * src + 1 - self.core, BRICK)], self.swsend.at[i], self.swrecv.at[i], self.tp, self.partner).wait()

    def end_line(self):
        for phase in range(2):
            role = self.role(phase)
            for kind in range(2):
                @pl.when(role == 1)
                def _():
                    @pl.loop(0, GROUPS)
                    def _(idx):
                        for way, to_role in enumerate((0, 2)):
                            self.result_copy(phase, kind, idx, way, to_role).wait_send()

                @pl.when(role == 2)
                def _():
                    @pl.loop(0, GROUPS)
                    def _(idx):
                        self.result_copy(phase, kind, idx, 0, 3).wait_send()

                @pl.when(role == 3)
                def _():
                    @pl.loop(0, GROUPS)
                    def _(idx):
                        self.result_copy(phase, kind, idx, 0, 2).wait_recv()

            for src in FAR_ROLES:
                @pl.when(role == src)
                def _():
                    for i in range(GROUPS):
                        self.act_copy(phase, src, i, self.plane(phase, 1)).wait_send()
                        self.w_copy(phase, src, i, self.plane(phase, 1)).wait_send()


    def brick(self, which, ref):
        return ref.at[:, pl.ds(0, TILE)] if which == DWKV else ref

    def pair_copy(self, kind, i, src, which=None):
        which = kind if which is None else which
        return hand_over(src, self.brick(kind, self.pland.at[which, i]), self.dsend.at[which, i], self.drecv.at[which, i], self.tp, self.partner)

    def chip_copies(self, which):
        return [hand_over(self.brick(which, self.keep.at[which % SLOTS, lax.div(peer, 2)]), self.brick(which, self.xland.at[which, n]),
                          self.xsend.at[which, n], self.xrecv.at[which, n], self.tp, peer) for n, peer in enumerate((self.x, self.y))]

    def half_copies(self, which):
        block = self.brick(which, self.keep.at[which % SLOTS, lax.div(self.diag, 2)])
        return [hand_over(block.at[win(n, TILE)], self.brick(which, self.hland.at[which, n]),
                          self.hsend.at[which, n], self.hrecv.at[which, n], self.tp, peer) for n, peer in enumerate((self.x, self.y))]

    def own_blocks(self):
        return [pltpu.make_async_copy(self.dkv.at[2 * i + self.core], self.keep.at[0, i], self.early.at[i]) for i in range(CHIPS)]

    def hand_dkv(self):
        for i in range(CHIPS):
            self.pair_copy(DKV, i, self.dkv.at[2 * i + 1 - self.core]).start()
        for copy in self.own_blocks():
            copy.start()

    def fetch(self, part):
        half, i = win(lax.rem(lax.div(part, CHIPS), 2), BRICK), lax.rem(part, CHIPS)
        narrow = pl.ds(0, TILE)
        for n, block in enumerate((2 * i + 1 - self.core, 2 * i + self.core)):
            block = win(block, BRICK)
            right = self.right.at[n]
            for kind, pair in enumerate((((self.o.at[:, half], self.left.at[n]), (self.g.at[:, block], right)),
                                         ((self.h.at[:, block], self.left.at[n]), (self.dq.at[:, half], right)),
                                         ((self.h.at[:, block], self.left.at[n]), (self.dkvb, right.at[:, narrow])))):
                @pl.when(lax.div(part, 2 * CHIPS) == kind)
                def _():
                    for m, (src, dst) in enumerate(pair):
                        pltpu.make_async_copy(src, dst, self.early.at[2 * n + m]).start()

    def make(self, part, which=None):
        kind, i = which, lax.rem(part, CHIPS)
        which = 1 + lax.div(part, CHIPS) if which is None else which
        col = pl.ds(0, BRICK if kind is None else TILE)
        slot = self.stage.at[lax.rem(part, 2), :, col]

        @pl.when(i > 1)
        def _():
            self.pair_copy(kind, i - 2, slot, which).wait_send()

        for n, dst in enumerate((slot, self.keep.at[lax.rem(which, SLOTS), i, :, col])):
            left, right = self.left.at[n], self.right.at[n, :, col]
            for m, factor in enumerate((left, right)):
                pltpu.make_async_copy(self.h.at[:, col] if m else self.h.at[:, win(0, BRICK)], factor, self.early.at[2 * n + m]).wait()
            dst[...] = dot(left[...], right[...], TN)
            if n == 0:
                self.pair_copy(kind, i, slot, which).start()

        @pl.when((part != PARTS - 1) & (part != PARTS + CHIPS - 1))
        def _():
            self.fetch(part + 1)

    def total(self, which, count, add):
        @pl.loop(0, count * HEADS)
        def _(step):
            add(lax.div(step, HEADS), win(lax.rem(step, HEADS), LANE // 2))

    def add_pair(self, which):
        keep = self.keep.at[which % SLOTS]
        landed = [self.brick(which, self.pland.at[which, i]) for i in range(CHIPS)]
        for i in range(CHIPS):
            self.pair_copy(which, i, landed[i]).wait_recv()
        for i in range(0 if which == DKV else CHIPS // 2, CHIPS):
            self.pair_copy(which, i, landed[i]).wait_send()
        if which == DKV:
            for copy in self.own_blocks():
                copy.wait()
            self.fetch(0)
        self.move([(landed[i], self.brick(which, self.tmp.at[i])) for i in range(CHIPS)])
        col = pl.ds(0, TILE if which == DWKV else BRICK)

        def add(i, row):
            keep[i, row, col] = keep[i, row, col] + self.tmp[i, row, col]

        self.total(which, CHIPS, add)
        for copy in self.half_copies(which):
            copy.start()

    def relay(self, which):
        for copy in self.half_copies(which):
            copy.wait()
        self.move([(self.brick(which, self.hland.at[which, n]), self.brick(which, self.tmp.at[n, win(0, TILE)])) for n in range(2)])
        col = pl.ds(0, TILE if which == DWKV else BRICK)
        for n, peer in enumerate((self.y, self.x)):
            block = self.keep.at[which % SLOTS, lax.div(peer, 2)]
            for step in range(CHIPS):
                row, src = win(CHIPS * n + step, LANE // 2), win(step, LANE // 2)
                block[row, col] = block[row, col] + self.tmp[n, src, col]
        for copy in self.chip_copies(which):
            copy.start()

    def place(self, which, owner):
        if which in DWO:
            return self.dwo.at[win(which - DWO[0], BRICK), win(owner, BRICK)]
        if which in DWQ:
            return self.dwq.at[win(owner, BRICK), win(which - DWQ[0], BRICK)]
        return self.dwkv.at[win(owner, BRICK)]

    def share_copy(self, which, kind):
        owner = (self.cp, self.cp, self.cp, self.x, self.y, self.y, self.x, self.diag, self.diag)[kind]
        to = (self.x, self.y, self.partner, self.partner, self.partner, self.x, self.y, self.partner, self.partner)[kind]
        place = self.place(which, owner)
        if kind > 4:
            place = place.at[win((kind + 1) % 2, TILE)]
        return hand_over(place, place, self.gsend.at[which, kind], self.grecv.at[which, kind], self.tp, to)

    def shared_place(self, which, kind):
        mate = lambda idx: plane_peers(idx)[-1]
        owner = (self.x, self.y, self.partner, mate(self.x), mate(self.y), self.diag, self.diag, mate(self.diag), mate(self.diag))[kind]
        place = self.place(which, owner)
        if kind > 4:
            place = place.at[win((kind + 1) % 2, TILE)]
        return hand_over(place, place, self.gsend.at[which, kind], self.grecv.at[which, kind], self.tp, self.partner)

    def add_chips(self, which):
        copies = self.chip_copies(which)
        for copy in copies:
            copy.wait()
        self.move([(self.brick(which, self.xland.at[which, n]), self.brick(which, self.tmp.at[n])) for n in range(len(copies))])
        col = pl.ds(0, TILE if which == DWKV else BRICK)
        own = self.keep.at[which % SLOTS, self.chip]

        def add(_, row):
            own[row, col] = own[row, col] + (self.tmp[0, row, col] + self.tmp[1, row, col])

        self.total(which, 1, add)
        if which == DKV:
            self.total(which, 1, self.keep_z)
            for end, inner in ((0, 1), (3, 2)):
                @pl.when(self.tp == end)
                def _():
                    self.z_copy(0, inner).start()
            return
        self.move([(self.brick(which, own), self.place(which, self.cp))])
        for kind in range(3):
            self.share_copy(which, kind).start()

    def pass_on(self, which):
        for kind in range(2):
            self.shared_place(which, kind).wait_recv()
        for kind in (5, 6, 3, 4):
            self.share_copy(which, kind).start()

    def pass_diagonal(self, which):
        for kind in (5, 6):
            self.shared_place(which, kind).wait_recv()
        for kind in (7, 8):
            self.share_copy(which, kind).start()

    def end_share(self, which):
        for kind in (2, 3, 4, 7, 8):
            self.shared_place(which, kind).wait_recv()
        for kind in range(9):
            self.share_copy(which, kind).wait_send()


    def keep_z(self, _, row):
        self.zbuf[row] = self.keep[0, self.chip, row]

    def z_copy(self, slot, to):
        return hand_over(self.zbuf, self.zland.at[slot], self.zsend.at[slot], self.zrecv.at[slot], to, self.cp)

    def z_result(self, slot, to):
        return hand_over(self.dkvb, self.dkvb, self.zsend.at[slot], self.zrecv.at[2], to, self.cp)

    def meet(self):
        for inner in (1, 2):
            @pl.when(self.tp == inner)
            def _():
                self.z_copy(0, CHIPS - 1 - inner).wait_recv()
                self.move([(self.zland.at[0], self.tmp.at[0])])

                def add(_, row):
                    self.zbuf[row] = self.zbuf[row] + self.tmp[0, row]

                self.total(DKV, 1, add)
                if inner == 2:
                    self.z_copy(1, 1).start()

    def settle(self):
        half = LANE // 2

        @pl.when(self.tp == 1)
        def _():
            self.z_copy(1, 2).wait_recv()
            self.move([(self.zland.at[1], self.tmp.at[0]), (self.tabs, self.tmp.at[1, win(0, LANE), win(0, LANE)])])
            for b in range(HEADS):
                cos, sin = self.tmp[1, win(0, half), win(0, LANE)], self.tmp[1, win(1, half), win(0, LANE)]
                for kind in range(2):
                    row, col = win(2 * kind + b // CHIPS, LANE), win(b % CHIPS, LANE)
                    part = self.zbuf[row, col] + self.tmp[0, row, col]
                    if kind == 0:
                        low, high = part[:half], part[half:]
                        part = jnp.concatenate([low * cos + high * sin, high * cos - low * sin], axis=0)
                    self.abuf[win(b, LANE), win(DEPTH // LANE + kind, LANE)] = part.T.astype(BF16)
            self.move([(self.abuf.at[:, pl.ds(DEPTH, TILE)], self.dkvb)])
            self.z_result(2, 2).start()
            self.z_result(0, 0).start()

    def take(self):
        @pl.when(self.tp == 2)
        def _():
            self.z_result(2, 1).wait_recv()
            self.z_result(2, 3).start()
            self.move([(self.dkvb, self.abuf.at[:, pl.ds(DEPTH, TILE)])])

    def get_result(self):
        for end in (0, 3):
            @pl.when(self.tp == end)
            def _():
                self.z_result(2, 1).wait_recv()
                self.z_copy(0, 1).wait_send()

        @pl.when(self.tp == 1)
        def _():
            self.z_result(0, 0).wait_send()

        @pl.when(self.tp == 2)
        def _():
            self.z_copy(1, 1).wait_send()

        @pl.when((self.tp == 1) | (self.tp == 2))
        def _():
            self.z_result(2, 3).wait_send()

        self.fetch(PARTS)


STEPS = {"add_pair": ((1, 3, 5, 7, 9, 22), (1, 5, 9, 13, 17, 23)), "relay": ((3, 6, 7, 10, 13, 24), (4, 8, 12, 16, 20, 25)),
         "add_chips": ((6, 10, 13, 15, 18, 26), (7, 11, 15, 19, 23, 28)), "pass_on": ((25, 26, 27, 28, 29), (15, 19, 23, 27, 30)),
         "pass_diagonal": ((28, 29, 30, 31, 31), (19, 23, 27, 31, 31))}
ONCE = {"hand_dkv": 0, "meet": 10, "settle": 15, "get_result": 17}
PARTS, LATE = 16, 18


def exchange_kernel(*refs):
    dev = Exchange(*refs)
    barrier = pltpu.get_barrier_semaphore()
    for step in range(1, CHIPS):
        pl.semaphore_signal(barrier, inc=1, device_id=(lax.rem(dev.tp + step, CHIPS), dev.cp), device_id_type=MESH)
    for peer in plane_peers(dev.cp):
        pl.semaphore_signal(barrier, inc=1, device_id=(dev.tp, peer), device_id_type=MESH)
    pl.semaphore_wait(barrier, 7)
    blocks = range(GROUPS)
    dev.feed(0, 3, blocks[:LEADS[0]], ())
    dev.feed(0, 0, blocks[:1], ())
    for i in blocks[1:]:
        dev.feed(0, 0, (i,), ())
        if i <= LEADS[1]:
            dev.feed(1, 3, (i - 1,), ())
    dev.feed(0, 0, (), blocks)
    dev.feed(0, 2, blocks, blocks)
    dev.feed(1, 2, blocks[:EARLY], ())
    dev.start_line()
    dev.end_swap()
    busy = dev.tp == 2

    @pl.loop(0, CHIPS * GROUPS)
    def _(now):
        idx = lax.rem(now, GROUPS)
        spans = [(lax.div(now, GROUPS) == 2 * phase + kind, phase, kind) for phase in range(2) for kind in range(2)]

        @pl.when(now == 2 * GROUPS)
        def _():
            dev.feed(1, 0, blocks, blocks)
            dev.feed(1, 2, blocks[EARLY:], blocks)
            dev.take()

        for here, phase, kind in spans:
            @pl.when(here)
            def _():
                if kind:
                    dev.swap_weights(phase, idx)
                else:
                    dev.group(phase, kind, idx)

        for step, at in ONCE.items():
            @pl.when(now == at)
            def _():
                getattr(dev, step)()

        for step, (early, late) in STEPS.items():
            for which in range(SETS - len(late), SETS):
                @pl.when(now == jnp.where(busy, early[which - SETS], late[which - SETS]))
                def _():
                    getattr(dev, step)(which)

        @pl.loop(jnp.where(busy, jnp.maximum(2 * now - 2, 0), jnp.maximum(now - 1, 0)), jnp.minimum(jnp.where(busy, 2 * now, now), PARTS))
        def _(part):
            dev.make(part)

        @pl.when((now >= LATE) & (now < LATE + CHIPS))
        def _():
            dev.make(now + PARTS - LATE, DWKV)

        for here, phase, kind in spans:
            if kind:
                @pl.when(here)
                def _():
                    dev.group(phase, kind, idx)

    for which in range(1, SETS):
        dev.end_share(which)
    dev.end_line()


def exchange(*operands):
    return pl.pallas_call(
        exchange_kernel,
        name="exchange",
        out_shape=[jax.ShapeDtypeStruct(*spec) for spec in OUTPUTS.values()],
        in_specs=[ANY] * len(operands),
        out_specs=[ANY] * len(OUTPUTS),
        scratch_shapes=[pltpu.VMEM(*spec) for spec in BUFFERS.values()] + [DMA(shape) for shape in SEMS.values()] + [pltpu.SemaphoreType.REGULAR((2,))],
        compiler_params=talking(1),
        cost_estimate=cost(300),
    )(*operands)


def finish_kernel(out_ref, dh_ref, dwo_ref, dwq_ref, dwkv_ref, out, dh, dwo, dwq, dwk, dwv):
    out[...] = out_ref[...]
    dh[...] = dh_ref[...]
    dwo[...] = dwo_ref[...]
    dwq[...] = dwq_ref[...].reshape(dwq.shape)
    dwk[...] = dwkv_ref[:, :LANE]
    dwv[...] = dwkv_ref[:, LANE:]


def finish(*arrays, steps=HEADS):
    heads = (DEPTH, HEADS, LANE)
    shapes = [(arrays[0].shape, BF16), (arrays[1].shape, BF16), (arrays[2].shape, F32), (heads, F32), ((DEPTH, LANE), F32), ((DEPTH, LANE), F32)]
    block = lambda shape: pl.BlockSpec((shape[0] // steps, *shape[1:]), lambda i: (i,) + (0,) * (len(shape) - 1))
    return pl.pallas_call(
        finish_kernel,
        name="finish",
        grid=(steps,),
        out_shape=[jax.ShapeDtypeStruct(*spec) for spec in shapes],
        in_specs=[block(a.shape) for a in arrays],
        out_specs=[block(shape) for shape, _ in shapes],
        compiler_params=pltpu.CompilerParams(vmem_limit_bytes=VMEM_CAP),
        cost_estimate=cost(1),
    )(*arrays)


def solution(mesh):
    def local_program(hidden, grad_out, w_query, w_key, w_value, w_out):
        tp, cp = lax.axis_index("tp"), lax.axis_index("cp")
        h, g = hidden.reshape(ROWS, DEPTH), grad_out.reshape(ROWS, DEPTH)
        q_scale = LANE ** -0.5
        tabs, cos_tab, sin_tab, mask = tables(cp)
        wo2 = w_out.reshape(ROWS, DEPTH)
        wq_t = turn(w_query)
        wo_half, wq_half = [lax.dynamic_slice(w, (lax.rem(cp, 2) * BRICK, 0), (BRICK, HALF_W)) for w in (wo2, wq_t)]
        one_way, other_way = jnp.where(tp <= 1, wo_half, wq_half), jnp.where(tp <= 1, wq_half, wo_half)
        near = lax.ppermute(one_way, "tp", [(0, 1), (3, 2)])
        mid = lax.ppermute(other_way, "tp", [(2, 1), (1, 2)])
        far = lax.ppermute(other_way, "tp", [(3, 1), (0, 2)])
        q, d_o, kv = projections(h, g, wq_t, wo2, w_key, w_value, cos_tab, sin_tab, q_scale)
        o, dq, dkv = attention(q, d_o, kv, mask, cos_tab, sin_tab, q_scale)
        out, dh, dwo, dwq, dwk, dwv = finish(*exchange(o, dq, wo2, wq_t, near, mid, far, w_key, w_value, g, h, dkv.reshape(HEADS, BRICK, BRICK), tabs)[:5])
        return out.reshape(hidden.shape), dh.reshape(hidden.shape), dwq, dwk, dwv, dwo.reshape(w_out.shape)

    row_spec, head_spec = P(None, "cp", None), P("tp", None, None)
    query_spec = P(None, "tp", None)
    return jax.shard_map(local_program, mesh=mesh, in_specs=(row_spec, row_spec, query_spec, P(), P(), head_spec),
                         out_specs=(row_spec, row_spec, query_spec, P(), P(), head_spec), check_vma=False)
```

```python
import functools
import jax
import jax.numpy as jnp
from jax import lax
from jax.experimental import pallas as pl
from jax.experimental.pallas import tpu as pltpu
from jax.sharding import PartitionSpec as P

ROWS, DEPTH, LANE, TILE, BRICK, HALF_W = 1024, 4096, 128, 256, 512, 2048
CHIPS, HEADS, GROUPS = 4, 8, 8
VMEM_CAP = 66_000_000
MESH = pl.DeviceIdType.MESH
F32, BF16 = jnp.float32, jnp.bfloat16
NT = (((1,), (1,)), ((), ()))
NN = (((1,), (0,)), ((), ()))
TN = (((0,), (0,)), ((), ()))
ANY = pl.BlockSpec(memory_space=pl.ANY)
VM = pl.BlockSpec(memory_space=pltpu.VMEM)
DMA = pltpu.SemaphoreType.DMA


def dot(lhs, rhs, dims=NN):
    return lax.dot_general(lhs, rhs, dims, preferred_element_type=F32)


def cost(gigaflops):
    return pl.CostEstimate(flops=gigaflops * 10 ** 9, bytes_accessed=10 ** 8, transcendentals=0)


def talking(collective_id):
    return pltpu.CompilerParams(collective_id=collective_id, has_side_effects=True, vmem_limit_bytes=VMEM_CAP)


def by_row(reduce, tile):
    return reduce(tile, axis=1, keepdims=True)


def twice(tile):
    return jnp.concatenate([tile, tile], axis=0)


def win(index, size):
    start = index * size
    return pl.ds(start if isinstance(start, int) else pl.multiple_of(start, size), size)


def plane_peers(cp):
    x_of = lambda idx: idx + 2 - CHIPS * lax.rem(lax.div(idx, 2), 2)
    y_of = lambda idx: lax.rem(idx + CHIPS, HEADS)
    return x_of(cp), y_of(cp), x_of(y_of(cp)), cp + 1 - 2 * lax.rem(cp, 2)


def hand_over(src, dst, send_sem, recv_sem, tp, cp):
    return pltpu.make_async_remote_copy(src, dst, send_sem, recv_sem, device_id=(tp, cp), device_id_type=MESH)


def rope(tile, cos, sin):
    heads = [tile[:, lo:lo + LANE] for lo in range(0, tile.shape[1], LANE)]
    return [one * cos + pltpu.roll(one, LANE // 2, 1) * sin for one in heads]


def proj_kernel(q_scale, h_ref, g_ref, wq_ref, wo_ref, wk_ref, wv_ref, cos_ref, sin_ref,
                q_out, do_out, kv_out, hbuf, gbuf, wqbuf, wobuf, wkvbuf, qbuf, dobuf, kvbuf,
                load_sem, wkv_sem, osem, send_sem, recv_sem):
    tp, cp = lax.axis_index("tp"), lax.axis_index("cp")
    peers = plane_peers(cp)
    *others, partner = peers
    barrier = pltpu.get_barrier_semaphore()
    for peer in peers:
        pl.semaphore_signal(barrier, inc=1, device_id=(tp, peer), device_id_type=MESH)
    rows = [win(i, TILE) for i in range(CHIPS)]
    loads_h, loads_g, loads_wq, loads_wo = [
        [pltpu.make_async_copy(src.at[r], dst.at[r], load_sem.at[which, i]) for i, r in enumerate(rows)]
        for which, (src, dst) in enumerate(((h_ref, hbuf), (g_ref, gbuf), (wq_ref, wqbuf), (wo_ref, wobuf)))]
    loads_kv = [pltpu.make_async_copy(src, wkvbuf.at[:, win(i, LANE)], wkv_sem.at[i]) for i, src in enumerate((wk_ref, wv_ref))]
    for copy in loads_h[:1] + loads_kv + loads_h[1:]:
        copy.start()
    for copy in loads_h[:1] + loads_kv:
        copy.wait()
    for copy in loads_wq:
        copy.start()
    cos, sin = twice(cos_ref[...]), twice(sin_ref[...])
    sends, stored = [], []

    def share(i):
        piece = kv_out.at[cp, rows[i]]
        stored[i].wait()
        sends.append([hand_over(piece, piece, send_sem.at[n, i], recv_sem.at[n, i], tp, peer) for n, peer in enumerate(peers)])
        for copy in sends[i]:
            copy.start()

    for i, row in enumerate(rows):
        if i:
            loads_h[i].wait()
        kv = dot(hbuf[row, :], wkvbuf[...])
        kvbuf[row, win(0, LANE)] = rope(kv[:, :LANE], cos, sin)[0].astype(BF16)
        kvbuf[row, win(1, LANE)] = kv[:, LANE:].astype(BF16)
        stored.append(pltpu.make_async_copy(kvbuf.at[row], kv_out.at[cp, row], osem.at[2 + i]))
        stored[i].start()
        if i == 0:
            pl.semaphore_wait(barrier, len(peers))
        else:
            share(i - 1)
    share(CHIPS - 1)
    for copy in loads_wq:
        copy.wait()
    for copy in loads_g + loads_wo:
        copy.start()
    cos2, sin2 = twice(cos), twice(sin)

    @pl.loop(0, HEADS)
    def _(step):
        row, col = win(lax.div(step, CHIPS), BRICK), win(lax.rem(step, CHIPS), TILE)
        tile = dot(hbuf[row, :], wqbuf[col, :], NT)
        qbuf[row, col] = (jnp.concatenate(rope(tile, cos2, sin2), axis=1) * q_scale).astype(BF16)

    store_q = pltpu.make_async_copy(qbuf, q_out, osem.at[0])
    store_q.start()
    for copy in loads_g + loads_wo:
        copy.wait()
    passes = []

    def pass_on(i):
        for n, peer in enumerate(others):
            sends[i][n].wait_recv()
            piece = kv_out.at[peer, rows[i]]
            copy = hand_over(piece, piece, send_sem.at[CHIPS + n, i], recv_sem.at[CHIPS + n, i], tp, partner)
            copy.start()
            passes.append(copy)

    for half in range(2):
        @pl.loop(half * CHIPS, (half + 1) * CHIPS)
        def _(step):
            row, col = win(lax.div(step, CHIPS), BRICK), win(lax.rem(step, CHIPS), TILE)
            dobuf[row, col] = dot(gbuf[row, :], wobuf[col, :], NT).astype(BF16)

        pass_on(half)
    store_do = pltpu.make_async_copy(dobuf, do_out, osem.at[1])
    store_do.start()
    for i in range(2, CHIPS):
        pass_on(i)
    for group in sends:
        group[-1].wait_recv()
        for copy in group:
            copy.wait_send()
    for copy in passes:
        copy.wait()
    store_q.wait()
    store_do.wait()


def turn_kernel(w_ref, out_ref):
    out_ref[...] = w_ref[...].reshape(BRICK, ROWS).T


def turn(w):
    return pl.pallas_call(
        turn_kernel,
        name="turn",
        grid=(GROUPS,),
        out_shape=jax.ShapeDtypeStruct((ROWS, DEPTH), BF16),
        in_specs=[pl.BlockSpec((BRICK, HEADS, LANE), lambda i: (i, 0, 0))],
        out_specs=pl.BlockSpec((ROWS, BRICK), lambda i: (0, i)),
        compiler_params=pltpu.CompilerParams(vmem_limit_bytes=VMEM_CAP),
        cost_estimate=cost(1),
    )(w)


def projections(h, g, wq_t, wo2, wk, wv, cos_tab, sin_tab, q_scale):
    square = (ROWS, ROWS)
    kv_shape = (HEADS, ROWS, TILE)
    return pl.pallas_call(
        functools.partial(proj_kernel, q_scale),
        name="projections",
        out_shape=[jax.ShapeDtypeStruct(s, BF16) for s in (square, square, kv_shape)],
        in_specs=[ANY] * 6 + [VM] * 2,
        out_specs=[ANY] * 3,
        scratch_shapes=[pltpu.VMEM(s, BF16) for s in [(ROWS, DEPTH)] * 4 + [(DEPTH, TILE), square, square, (ROWS, TILE)]]
        + [DMA(s) for s in ((CHIPS, CHIPS), (2,), (6,), (7, CHIPS), (7, CHIPS))],
        compiler_params=talking(0),
        cost_estimate=cost(20),
    )(h, g, wq_t, wo2, wk, wv, cos_tab, sin_tab)


def attn_kernel(q_scale, q_ref, do_ref, kv_ref, mask_ref, cos_ref, sin_ref, o_ref, dq_ref, dkv_ref):
    keys = kv_ref[:, :, :LANE].reshape(ROWS, LANE)
    vals = kv_ref[:, :, LANE:].reshape(ROWS, LANE)
    cos, sin, mask = twice(cos_ref[...]), twice(sin_ref[...]), twice(mask_ref[...])
    sums = []
    for pair in range(CHIPS):
        cols = [win(2 * pair + i, LANE) for i in range(2)]
        q = jnp.concatenate([q_ref[:, c] for c in cols], axis=0)
        do = jnp.concatenate([do_ref[:, c] for c in cols], axis=0)
        scores = dot(q, keys, NT) + mask
        prob = jnp.exp(scores - by_row(jnp.max, scores))
        prob = prob * (1.0 / by_row(jnp.sum, prob))
        prob_b = prob.astype(BF16)
        out = dot(prob_b, vals).astype(BF16)
        delta = by_row(jnp.sum, do.astype(F32) * out.astype(F32))
        d_score = (prob * (dot(do, vals, NT) - delta)).astype(BF16)
        dq = dot(d_score, keys)
        dq = ((dq * cos - pltpu.roll(dq, LANE // 2, 1) * sin) * q_scale).astype(BF16)
        for i, c in enumerate(cols):
            o_ref[:, c] = out[i * LANE:(i + 1) * LANE]
            dq_ref[:, c] = dq[i * LANE:(i + 1) * LANE]
        sums.append((dot(q.T, d_score), dot(do.T, prob_b)))
    for kind, parts in enumerate(zip(*sums)):
        total = (parts[0] + parts[1]) + (parts[2] + parts[3])
        for j in range(HEADS):
            dkv_ref[j, kind] = total[:, j * LANE:(j + 1) * LANE]


def attention(q, do, kv, mask, cos_tab, sin_tab, q_scale):
    row_block = pl.BlockSpec((LANE, ROWS), lambda b: (b, 0))
    whole = lambda a: pl.BlockSpec(a.shape, lambda b: (0,) * a.ndim)
    return pl.pallas_call(
        functools.partial(attn_kernel, q_scale),
        name="attention",
        grid=(HEADS,),
        out_shape=[jax.ShapeDtypeStruct((ROWS, ROWS), BF16)] * 2 + [jax.ShapeDtypeStruct((HEADS, 2, TILE, BRICK), F32)],
        in_specs=[row_block, row_block, pl.BlockSpec((HEADS, LANE, TILE), lambda b: (0, b, 0)), whole(mask), whole(cos_tab), whole(sin_tab)],
        out_specs=[row_block, row_block, pl.BlockSpec((HEADS, 2, LANE, LANE), lambda b: (0, 0, lax.div(b, CHIPS), lax.rem(b, CHIPS)))],
        compiler_params=pltpu.CompilerParams(vmem_limit_bytes=VMEM_CAP),
        cost_estimate=cost(30),
    )(q, do, kv, mask, cos_tab, sin_tab)


def tables(cp):
    half = LANE // 2
    pos = cp * LANE + jnp.arange(LANE)
    inv_freq = 1.0 / jnp.power(10000.0, jnp.arange(half, dtype=F32) * (2.0 / LANE))
    ang = pos.astype(F32)[:, None] * inv_freq[None, :]
    cos, sin = jnp.cos(ang), jnp.sin(ang)
    mask = jnp.where(jnp.arange(ROWS)[None, :] <= pos[:, None], 0.0, -jnp.inf).astype(F32)
    return jnp.concatenate([cos.T, sin.T], axis=0), jnp.concatenate([cos, cos], axis=1), jnp.concatenate([-sin, sin], axis=1), mask


DKV, DWO, DWQ, DWKV = 0, (1, 2), (3, 4), 5
SETS, SLOTS = 6, 5
LEADS, EARLY = (3, 2), 3
LATER = (5, 6, 7, )
FAR_ROLES = (0, 2, 3)
PHASES, SOURCES = 2, len(FAR_ROLES)
INPUTS = ("o", "dq", "wo", "wq", "near", "mid", "far", "wk", "wv", "g", "h", "dkv", "tabs")
OUTPUTS = {"out": ((ROWS, DEPTH), BF16), "dh": ((ROWS, DEPTH), BF16), "dwo": ((ROWS, DEPTH), F32), "dwq": ((DEPTH, ROWS), F32),
           "dwkv": ((DEPTH, TILE), F32), "dkvb": ((ROWS, TILE), BF16), "wland": ((DEPTH, HALF_W), BF16),
           "pland": ((SETS, CHIPS, BRICK, BRICK), F32), "xland": ((SETS, PHASES, BRICK, BRICK), F32), "hland": ((SETS, PHASES, TILE, BRICK), F32), "zland": ((PHASES, BRICK, BRICK), F32)}
BUFFERS = {"abuf": ((ROWS, DEPTH + TILE), BF16), "wa": ((DEPTH, HALF_W), BF16), "wb": ((DEPTH, TILE), BF16), "wkv": ((DEPTH, TILE), BF16),
           "tile_a": ((LANE, HALF_W), BF16), "tile_b": ((ROWS, TILE), BF16), "keep": ((SLOTS, CHIPS, BRICK, BRICK), F32),
           "tmp": ((CHIPS, BRICK, BRICK), F32), "stage": ((PHASES, BRICK, BRICK), F32), "left": ((PHASES, ROWS, BRICK), BF16),
           "right": ((PHASES, ROWS, BRICK), BF16), "zbuf": ((BRICK, BRICK), F32)}
SEMS = {"load": (12,), "early": (CHIPS,), "held": (CHIPS,), "asend": (PHASES, GROUPS), "arecv": (PHASES, SOURCES, GROUPS), "wsend": (PHASES, GROUPS), "wrecv": (PHASES, SOURCES, GROUPS), "fsend": (PHASES, SOURCES), "frecv": (PHASES, SOURCES, GROUPS),
        "rsend": (PHASES, PHASES, PHASES, GROUPS), "rrecv": (PHASES, PHASES, GROUPS), "swsend": (SOURCES,), "swrecv": (SOURCES,), "dsend": (SETS, CHIPS), "drecv": (SETS, CHIPS),
        "xsend": (SETS, PHASES), "xrecv": (SETS, PHASES), "hsend": (SETS, PHASES), "hrecv": (SETS, PHASES), "zsend": (SOURCES,), "zrecv": (SOURCES,), "gsend": (SETS, 9), "grecv": (SETS, 9)}


class Exchange:
    def __init__(self, *refs):
        for name, ref in zip((*INPUTS, *OUTPUTS, *BUFFERS, *SEMS, "credit"), refs):
            setattr(self, name, ref)
        self.tp, self.cp = lax.axis_index("tp"), lax.axis_index("cp")
        self.core, self.chip = lax.rem(self.cp, 2), lax.div(self.cp, 2)
        self.x, self.y, self.diag, self.partner = plane_peers(self.cp)
        self.acts, self.weights, self.results = (self.o, self.dq), (self.wo, self.wq), (self.out, self.dh)

    def move(self, pairs):
        copies = [pltpu.make_async_copy(src, dst, self.load.at[i]) for i, (src, dst) in enumerate(pairs)]
        for copy in copies:
            copy.start()
        for copy in copies:
            copy.wait()


    def plane(self, phase, role):
        return CHIPS - 1 - role if phase else role

    def role(self, phase):
        return self.plane(phase, self.tp)

    def act_copy(self, phase, src, i, to):
        row = win(i, LANE)
        return hand_over(self.acts[phase].at[row], self.abuf.at[row, win(src, ROWS)], self.asend.at[phase, i],
                         self.arecv.at[phase, FAR_ROLES.index(src), i], to, self.cp)

    def w_copy(self, phase, src, n, to):
        rows = 2 * src + self.core
        return hand_over(self.weights[phase].at[win(self.core, BRICK), win(GROUPS + n, TILE)], self.wland.at[win(rows, BRICK), win(n, TILE)],
                         self.wsend.at[phase, n], self.wrecv.at[phase, FAR_ROLES.index(src), n], to, self.cp)

    def cross_copy(self, phase, src, n, core):
        place = self.wland.at[win(2 * src + core, BRICK), win(n, TILE)]
        slot = FAR_ROLES.index(src)
        return hand_over(place, place, self.fsend.at[phase, slot], self.frecv.at[phase, slot, n], self.tp, self.partner)

    def piece(self, phase, kind, idx):
        if kind:
            return self.results[phase].at[:, win(GROUPS + idx, TILE)]
        return self.results[phase].at[win(idx, LANE), win(0, HALF_W)]

    def result_copy(self, phase, kind, idx, way, to_role):
        piece = self.piece(phase, kind, idx)
        return hand_over(piece, piece, self.rsend.at[phase, way, kind, idx], self.rrecv.at[phase, kind, idx], self.plane(phase, to_role), self.cp)

    def ask_far(self, phase):
        pl.semaphore_signal(self.credit.at[phase], inc=1, device_id=(self.plane(phase, 3), self.cp), device_id_type=MESH)

    def multiply(self, phase, kind, idx):
        weight = self.weights[phase]

        def product(row, weights, col):
            total = dot(self.abuf[row, pl.ds(0, DEPTH)], weights)
            if phase:
                total = total + dot(self.abuf[row, pl.ds(DEPTH, TILE)], self.wkv[col, :], NT)
            return total.astype(BF16)

        if kind == 0:
            row = win(idx, LANE)
            for src in FAR_ROLES:
                self.act_copy(phase, src, idx, self.plane(phase, src)).wait_recv()
            self.ask_far(phase)

            @pl.loop(0, CHIPS)
            def _(i):
                col = win(i, BRICK)
                self.tile_a[:, col] = product(row, self.wa[:, col], col)
        else:
            for src in FAR_ROLES:
                self.cross_copy(phase, src, idx, 1 - self.core).wait_recv()
                self.cross_copy(phase, src, idx, self.core).wait_send()
            pairs = [(self.wland.at[win(src, ROWS), win(idx, TILE)], self.wb.at[win(src, ROWS)]) for src in FAR_ROLES]
            pairs.append((weight.at[:, win(GROUPS + idx, TILE)], self.wb.at[win(1, ROWS)]))
            self.move(pairs)

            @pl.loop(0, CHIPS)
            def _(i):
                row = win(i, TILE)
                self.tile_b[row, :] = product(row, self.wb[...], win(GROUPS + idx, TILE))

        self.move([(self.tile_b if kind else self.tile_a, self.piece(phase, kind, idx))])
        for way, to_role in enumerate((0, 2)):
            self.result_copy(phase, kind, idx, way, to_role).start()

    def swap_weights(self, phase, idx):
        @pl.when(self.role(phase) == 1)
        def _():
            for src in FAR_ROLES:
                self.w_copy(phase, src, idx, self.plane(phase, src)).wait_recv()
                self.cross_copy(phase, src, idx, self.core).start()

            @pl.when(idx < GROUPS - LEADS[phase])
            def _():
                self.ask_far(phase)

    def group(self, phase, kind, idx):
        role = self.role(phase)

        @pl.when(role == 0)
        def _():
            self.result_copy(phase, kind, idx, 0, 1).wait_recv()

        @pl.when(role == 1)
        def _():
            self.multiply(phase, kind, idx)

        @pl.when(role == 2)
        def _():
            self.result_copy(phase, kind, idx, 0, 1).wait_recv()
            self.result_copy(phase, kind, idx, 0, 3).start()

        item = idx + LEADS[phase]

        @pl.when((role == 3) & ((item < GROUPS) | (kind == 0)))
        def _():
            pl.semaphore_wait(self.credit.at[phase], 1)

            @pl.when((item < GROUPS) & (kind == 0))
            def _():
                self.act_copy(phase, 3, item, self.plane(phase, 1)).start()

            @pl.when((item >= GROUPS) | (kind == 1))
            def _():
                self.w_copy(phase, 3, lax.rem(item, GROUPS), self.plane(phase, 1)).start()

    def feed(self, phase, src, acts, weights):
        @pl.when(self.role(phase) == src)
        def _():
            for i in acts:
                self.act_copy(phase, src, i, self.plane(phase, 1)).start()
            for n in weights:
                self.w_copy(phase, src, n, self.plane(phase, 1)).start()

    def start_line(self):
        for phase in range(PHASES):
            @pl.when(self.role(phase) == 1)
            def _():
                swaps = []
                for i, (half, src) in enumerate(zip((self.near, self.mid, self.far), FAR_ROLES)):
                    swaps.append(hand_over(half, self.wa.at[win(2 * src + self.core, BRICK)], self.swsend.at[i], self.swrecv.at[i], self.tp, self.partner))
                    swaps[i].start()
                pairs = [(half, self.wa.at[win(2 * src + self.core, BRICK)]) for half, src in zip((self.near, self.mid, self.far), FAR_ROLES)]
                pairs.append((self.weights[phase].at[:, win(0, HALF_W)], self.wa.at[win(1, ROWS)]))
                pairs.append((self.acts[phase], self.abuf.at[:, win(1, ROWS)]))
                pairs += [(src, self.wkv.at[:, win(i, LANE)]) for i, src in enumerate((self.wk, self.wv))]
                self.move(pairs)

    def end_swap(self):
        @pl.when((self.tp == 1) | (self.tp == 2))
        def _():
            for i, (half, src) in enumerate(zip((self.near, self.mid, self.far), FAR_ROLES)):
                hand_over(half, self.wa.at[win(2 * src + 1 - self.core, BRICK)], self.swsend.at[i], self.swrecv.at[i], self.tp, self.partner).wait()

    def end_line(self):
        for phase in range(PHASES):
            role = self.role(phase)
            for kind in range(PHASES):
                @pl.when(role == 1)
                def _():
                    @pl.loop(0, GROUPS)
                    def _(idx):
                        for way, to_role in enumerate((0, 2)):
                            self.result_copy(phase, kind, idx, way, to_role).wait_send()

                @pl.when(role == 2)
                def _():
                    @pl.loop(0, GROUPS)
                    def _(idx):
                        self.result_copy(phase, kind, idx, 0, 3).wait_send()

                @pl.when(role == 3)
                def _():
                    @pl.loop(0, GROUPS)
                    def _(idx):
                        self.result_copy(phase, kind, idx, 0, 2).wait_recv()

            for src in FAR_ROLES:
                @pl.when(role == src)
                def _():
                    for i in range(GROUPS):
                        self.act_copy(phase, src, i, self.plane(phase, 1)).wait_send()
                        self.w_copy(phase, src, i, self.plane(phase, 1)).wait_send()


    def brick(self, which, ref):
        return ref.at[:, pl.ds(0, TILE)] if which == DWKV else ref

    def pair_copy(self, kind, i, src, which=None):
        which = kind if which is None else which
        return hand_over(src, self.brick(kind, self.pland.at[which, i]), self.dsend.at[which, i], self.drecv.at[which, i], self.tp, self.partner)

    def chip_copies(self, which):
        return [hand_over(self.brick(which, self.keep.at[which % SLOTS, lax.div(peer, 2)]), self.brick(which, self.xland.at[which, n]),
                          self.xsend.at[which, n], self.xrecv.at[which, n], self.tp, peer) for n, peer in enumerate((self.x, self.y))]

    def half_copies(self, which):
        block = self.brick(which, self.keep.at[which % SLOTS, lax.div(self.diag, 2)])
        return [hand_over(block.at[win(n, TILE)], self.brick(which, self.hland.at[which, n]),
                          self.hsend.at[which, n], self.hrecv.at[which, n], self.tp, peer) for n, peer in enumerate((self.x, self.y))]

    def own_blocks(self):
        return [pltpu.make_async_copy(self.dkv.at[2 * i + self.core], self.keep.at[0, i], self.held.at[i]) for i in range(CHIPS)]

    def hand_dkv(self):
        for i in range(CHIPS):
            self.pair_copy(DKV, i, self.dkv.at[2 * i + 1 - self.core]).start()
        for copy in self.own_blocks():
            copy.start()
        self.fetch(0)

    def fetch(self, part):
        half, i = win(lax.rem(lax.div(part, CHIPS), 2), BRICK), lax.rem(part, CHIPS)
        narrow = pl.ds(0, TILE)
        for n, block in enumerate((2 * i + 1 - self.core, 2 * i + self.core)):
            block = win(block, BRICK)
            right = self.right.at[n]
            for kind, pair in enumerate((((self.o.at[:, half], self.left.at[n]), (self.g.at[:, block], right)),
                                         ((self.h.at[:, block], self.left.at[n]), (self.dq.at[:, half], right)),
                                         ((self.h.at[:, block], self.left.at[n]), (self.dkvb, right.at[:, narrow])))):
                @pl.when(lax.div(part, 2 * CHIPS) == kind)
                def _():
                    for m, (src, dst) in enumerate(pair):
                        pltpu.make_async_copy(src, dst, self.early.at[2 * n + m]).start()

    def make(self, part, which=None):
        kind, i = which, lax.rem(part, CHIPS)
        which = 1 + lax.div(part, CHIPS) if which is None else which
        col = pl.ds(0, BRICK if kind is None else TILE)
        slot = self.stage.at[lax.rem(part, 2), :, col]

        before = part - 2

        @pl.when((before >= 0) & (before < PARTS))
        def _():
            self.pair_copy(None, lax.rem(before, CHIPS), self.stage.at[0], 1 + lax.div(before, CHIPS)).wait_send()

        @pl.when(before >= PARTS)
        def _():
            self.pair_copy(DWKV, before - PARTS, self.brick(DWKV, self.stage.at[0])).wait_send()

        for n, dst in enumerate((slot, self.keep.at[lax.rem(which, SLOTS), i, :, col])):
            left, right = self.left.at[n], self.right.at[n, :, col]
            for m, factor in enumerate((left, right)):
                pltpu.make_async_copy(self.h.at[:, col] if m else self.h.at[:, win(0, BRICK)], factor, self.early.at[2 * n + m]).wait()
            dst[...] = dot(left[...], right[...], TN)
            if n == 0:
                self.pair_copy(kind, i, slot, which).start()

        @pl.when((part != PARTS - 1) & (part != PARTS + CHIPS - 1))
        def _():
            self.fetch(part + 1)

    def total(self, which, count, add):
        @pl.loop(0, count * HEADS)
        def _(step):
            add(lax.div(step, HEADS), win(lax.rem(step, HEADS), LANE // 2))

    def add_pair(self, which):
        keep = self.keep.at[which % SLOTS]
        landed = [self.brick(which, self.pland.at[which, i]) for i in range(CHIPS)]
        for i in range(CHIPS):
            self.pair_copy(which, i, landed[i]).wait_recv()
        for i in range({DKV: 0, DWKV: 2}.get(which, CHIPS), CHIPS):
            self.pair_copy(which, i, landed[i]).wait_send()
        if which == DKV:
            for copy in self.own_blocks():
                copy.wait()
        self.move([(landed[i], self.brick(which, self.tmp.at[i])) for i in range(CHIPS)])
        col = pl.ds(0, TILE if which == DWKV else BRICK)

        def add(i, row):
            keep[i, row, col] = keep[i, row, col] + self.tmp[i, row, col]

        self.total(which, CHIPS, add)
        for copy in self.half_copies(which):
            copy.start()

    def relay(self, which):
        for copy in self.half_copies(which):
            copy.wait()
        self.move([(self.brick(which, self.hland.at[which, n]), self.brick(which, self.tmp.at[n, win(0, TILE)])) for n in range(2)])
        col = pl.ds(0, TILE if which == DWKV else BRICK)
        for n, peer in enumerate((self.y, self.x)):
            block = self.keep.at[which % SLOTS, lax.div(peer, 2)]
            for step in range(CHIPS):
                row, src = win(CHIPS * n + step, LANE // 2), win(step, LANE // 2)
                block[row, col] = block[row, col] + self.tmp[n, src, col]
        for copy in self.chip_copies(which):
            copy.start()

    def place(self, which, owner):
        if which in DWO:
            return self.dwo.at[win(which - DWO[0], BRICK), win(owner, BRICK)]
        if which in DWQ:
            return self.dwq.at[win(owner, BRICK), win(which - DWQ[0], BRICK)]
        return self.dwkv.at[win(owner, BRICK)]

    def share_copy(self, which, kind):
        owner = (self.cp, self.cp, self.cp, self.x, self.y, self.y, self.x, self.diag, self.diag)[kind]
        to = (self.x, self.y, self.partner, self.partner, self.partner, self.x, self.y, self.partner, self.partner)[kind]
        place = self.place(which, owner)
        if kind > 4:
            place = place.at[win((kind + 1) % 2, TILE)]
        return hand_over(place, place, self.gsend.at[which, kind], self.grecv.at[which, kind], self.tp, to)

    def shared_place(self, which, kind):
        mate = lambda idx: plane_peers(idx)[-1]
        owner = (self.x, self.y, self.partner, mate(self.x), mate(self.y), self.diag, self.diag, mate(self.diag), mate(self.diag))[kind]
        place = self.place(which, owner)
        if kind > 4:
            place = place.at[win((kind + 1) % 2, TILE)]
        return hand_over(place, place, self.gsend.at[which, kind], self.grecv.at[which, kind], self.tp, self.partner)

    def add_chips(self, which):
        copies = self.chip_copies(which)
        for copy in copies:
            copy.wait()
        self.move([(self.brick(which, self.xland.at[which, n]), self.brick(which, self.tmp.at[n])) for n in range(len(copies))])
        col = pl.ds(0, TILE if which == DWKV else BRICK)
        own = self.keep.at[which % SLOTS, self.chip]

        def add(_, row):
            own[row, col] = own[row, col] + (self.tmp[0, row, col] + self.tmp[1, row, col])

        self.total(which, 1, add)
        if which == DKV:
            self.total(which, 1, self.keep_z)
            for end, inner in ((0, 1), (3, 2)):
                @pl.when(self.tp == end)
                def _():
                    self.z_copy(0, inner).start()
            return
        self.move([(self.brick(which, own), self.place(which, self.cp))])
        for kind in range(3):
            self.share_copy(which, kind).start()

    def pass_on(self, which):
        for kind in range(PHASES):
            self.shared_place(which, kind).wait_recv()
        for kind in (5, 6, 3, 4):
            self.share_copy(which, kind).start()

    def pass_diagonal(self, which):
        for kind in (5, 6):
            self.shared_place(which, kind).wait_recv()
        for kind in (7, 8):
            self.share_copy(which, kind).start()

    def end_share(self, which):
        for kind in (2, 3, 4, 7, 8):
            self.shared_place(which, kind).wait_recv()
        for kind in range(9):
            self.share_copy(which, kind).wait_send()


    def keep_z(self, _, row):
        self.zbuf[row] = self.keep[0, self.chip, row]

    def z_copy(self, slot, to):
        return hand_over(self.zbuf, self.zland.at[slot], self.zsend.at[slot], self.zrecv.at[slot], to, self.cp)

    def z_result(self, slot, to):
        return hand_over(self.dkvb, self.dkvb, self.zsend.at[slot], self.zrecv.at[2], to, self.cp)

    def meet(self):
        for inner in (1, 2):
            @pl.when(self.tp == inner)
            def _():
                self.z_copy(0, CHIPS - 1 - inner).wait_recv()
                self.move([(self.zland.at[0], self.tmp.at[0])])

                def add(_, row):
                    self.zbuf[row] = self.zbuf[row] + self.tmp[0, row]

                self.total(DKV, 1, add)
                if inner == 2:
                    self.z_copy(1, 1).start()
                    self.feed(0, 2, (), LATER)

    def settle(self):
        half = LANE // 2

        @pl.when(self.tp == 1)
        def _():
            self.z_copy(1, 2).wait_recv()
            self.move([(self.zland.at[1], self.tmp.at[0]), (self.tabs, self.tmp.at[1, win(0, LANE), win(0, LANE)])])
            for b in range(HEADS):
                cos, sin = self.tmp[1, win(0, half), win(0, LANE)], self.tmp[1, win(1, half), win(0, LANE)]
                for kind in range(PHASES):
                    row, col = win(2 * kind + b // CHIPS, LANE), win(b % CHIPS, LANE)
                    part = self.zbuf[row, col] + self.tmp[0, row, col]
                    if kind == 0:
                        low, high = part[:half], part[half:]
                        part = jnp.concatenate([low * cos + high * sin, high * cos - low * sin], axis=0)
                    self.abuf[win(b, LANE), win(DEPTH // LANE + kind, LANE)] = part.T.astype(BF16)
            self.move([(self.abuf.at[:, pl.ds(DEPTH, TILE)], self.dkvb)])
            self.z_result(2, 2).start()
            self.z_result(0, 0).start()

    def take(self):
        @pl.when(self.tp == 2)
        def _():
            self.z_result(2, 1).wait_recv()
            self.z_result(2, 3).start()
            self.move([(self.dkvb, self.abuf.at[:, pl.ds(DEPTH, TILE)])])

    def get_result(self):
        for end in (0, 3):
            @pl.when(self.tp == end)
            def _():
                self.z_result(2, 1).wait_recv()
                self.z_copy(0, 1).wait_send()

        @pl.when(self.tp == 1)
        def _():
            self.z_result(0, 0).wait_send()

        @pl.when(self.tp == 2)
        def _():
            self.z_copy(1, 1).wait_send()

        @pl.when((self.tp == 1) | (self.tp == 2))
        def _():
            self.z_result(2, 3).wait_send()


STEPS = {"add_pair": ((1, 3, 5, 9, 9, 22), (2, 5, 5, 7, 11, 27)),
         "relay": ((2, 5, 11, 12, 14, 26), (3, 9, 14, 11, 12, 28)),
         "add_chips": ((9, 9, 14, 21, 23, 30), (6, 12, 21, 21, 16, 30)),
         "pass_on": ((19, 25, 27, 26, 31), (17, 25, 29, 20, 31)),
         "pass_diagonal": ((27, 28, 30, 31, 31), (21, 29, 31, 24, 31))}
ONCE = {"hand_dkv": 0, "meet": 10, "get_result": 17}
PARTS, LATE = 16, (18, 18)
TURN, TURNS, NEAR, MID = 13, (13, 16, 13, 14), (10, 20), (16, 16)


def exchange_kernel(*refs):
    dev = Exchange(*refs)
    barrier = pltpu.get_barrier_semaphore()
    for step in range(1, CHIPS):
        pl.semaphore_signal(barrier, inc=1, device_id=(lax.rem(dev.tp + step, CHIPS), dev.cp), device_id_type=MESH)
    for peer in plane_peers(dev.cp):
        pl.semaphore_signal(barrier, inc=1, device_id=(dev.tp, peer), device_id_type=MESH)
    pl.semaphore_wait(barrier, 7)
    blocks = range(GROUPS)
    dev.feed(0, 3, blocks[:LEADS[0]], ())
    dev.feed(0, 0, blocks[:1], ())
    for i in blocks[1:]:
        dev.feed(0, 0, (i,), ())
        if i <= LEADS[1]:
            dev.feed(1, 3, (i - 1,), ())
    dev.feed(0, 0, (), blocks)
    dev.feed(0, 2, blocks, blocks[:GROUPS - len(LATER)])
    dev.feed(1, 2, blocks[:EARLY], ())
    dev.start_line()
    dev.end_swap()
    busy = dev.tp == 2

    @pl.loop(0, CHIPS * GROUPS)
    def _(now):
        turn = TURNS[0]
        for plane, own_turn in enumerate(TURNS):
            turn = jnp.where(dev.tp == plane, own_turn, turn)
        ahead = now - turn
        job = jnp.where(lax.rem(ahead, 2) == 0, 2 * GROUPS, turn) + lax.div(ahead, 2)
        job = jnp.where((ahead >= 0) & (now + turn < CHIPS * GROUPS), job, now)
        idx = lax.rem(job, GROUPS)
        spans = [(lax.div(job, GROUPS) == 2 * phase + kind, phase, kind) for phase in range(PHASES) for kind in range(PHASES)]

        for slots, src, acts in ((NEAR, 0, blocks), (MID, 2, blocks[EARLY:])):
            for slot, operands in zip(slots, ((acts, ()), ((), blocks))):
                @pl.when(now == slot)
                def _():
                    dev.feed(1, src, *operands)

        @pl.when(now == TURN)
        def _():
            dev.settle()
            dev.take()

        for here, phase, kind in spans:
            @pl.when(here)
            def _():
                if kind:
                    dev.swap_weights(phase, idx)
                else:
                    dev.group(phase, kind, idx)

        for step, at in ONCE.items():
            @pl.when(now == at)
            def _():
                getattr(dev, step)()

        for step, (early, late) in STEPS.items():
            for which in range(SETS - len(late), SETS):
                @pl.when(now == jnp.where(busy, early[which - SETS], late[which - SETS]))
                def _():
                    getattr(dev, step)(which)

        @pl.loop(jnp.clip(2 * now - 2, 0, PARTS), jnp.clip(2 * now, 0, PARTS))
        def _(part):
            dev.make(part)

        late = now - jnp.where(busy, *LATE)

        @pl.when(late == 0)
        def _():
            dev.fetch(PARTS)

        @pl.when((late >= 0) & (late < CHIPS))
        def _():
            dev.make(late + PARTS, DWKV)

        for here, phase, kind in spans:
            if kind:
                @pl.when(here)
                def _():
                    dev.group(phase, kind, idx)

    for which in range(1, SETS):
        dev.end_share(which)
    dev.end_line()


def exchange(*operands):
    return pl.pallas_call(
        exchange_kernel,
        name="exchange",
        out_shape=[jax.ShapeDtypeStruct(*spec) for spec in OUTPUTS.values()],
        in_specs=[ANY] * len(operands),
        out_specs=[ANY] * len(OUTPUTS),
        scratch_shapes=[pltpu.VMEM(*spec) for spec in BUFFERS.values()] + [DMA(shape) for shape in SEMS.values()] + [pltpu.SemaphoreType.REGULAR((2,))],
        compiler_params=talking(1),
        cost_estimate=cost(300),
    )(*operands)


def finish_kernel(out_ref, dh_ref, dwo_ref, dwq_ref, dwkv_ref, out, dh, dwo, dwq, dwk, dwv):
    out[...] = out_ref[...]
    dh[...] = dh_ref[...]
    dwo[...] = dwo_ref[...]
    dwq[...] = dwq_ref[...].reshape(dwq.shape)
    dwk[...] = dwkv_ref[:, :LANE]
    dwv[...] = dwkv_ref[:, LANE:]


def finish(*arrays, steps=HEADS):
    heads = (DEPTH, HEADS, LANE)
    shapes = [(arrays[0].shape, BF16), (arrays[1].shape, BF16), (arrays[2].shape, F32), (heads, F32), ((DEPTH, LANE), F32), ((DEPTH, LANE), F32)]
    block = lambda shape: pl.BlockSpec((shape[0] // steps, *shape[1:]), lambda i: (i,) + (0,) * (len(shape) - 1))
    return pl.pallas_call(
        finish_kernel,
        name="finish",
        grid=(steps,),
        out_shape=[jax.ShapeDtypeStruct(*spec) for spec in shapes],
        in_specs=[block(a.shape) for a in arrays],
        out_specs=[block(shape) for shape, _ in shapes],
        compiler_params=pltpu.CompilerParams(vmem_limit_bytes=VMEM_CAP),
        cost_estimate=cost(1),
    )(*arrays)


def solution(mesh):
    def local_program(hidden, grad_out, w_query, w_key, w_value, w_out):
        tp, cp = lax.axis_index("tp"), lax.axis_index("cp")
        h, g = hidden.reshape(ROWS, DEPTH), grad_out.reshape(ROWS, DEPTH)
        q_scale = LANE ** -0.5
        tabs, cos_tab, sin_tab, mask = tables(cp)
        wo2 = w_out.reshape(ROWS, DEPTH)
        wq_t = turn(w_query)
        wo_half, wq_half = [lax.dynamic_slice(w, (lax.rem(cp, 2) * BRICK, 0), (BRICK, HALF_W)) for w in (wo2, wq_t)]
        one_way, other_way = jnp.where(tp <= 1, wo_half, wq_half), jnp.where(tp <= 1, wq_half, wo_half)
        near = lax.ppermute(one_way, "tp", [(0, 1), (3, 2)])
        mid = lax.ppermute(other_way, "tp", [(2, 1), (1, 2)])
        far = lax.ppermute(other_way, "tp", [(3, 1), (0, 2)])
        q, d_o, kv = projections(h, g, wq_t, wo2, w_key, w_value, cos_tab, sin_tab, q_scale)
        o, dq, dkv = attention(q, d_o, kv, mask, cos_tab, sin_tab, q_scale)
        out, dh, dwo, dwq, dwk, dwv = finish(*exchange(o, dq, wo2, wq_t, near, mid, far, w_key, w_value, g, h, dkv.reshape(HEADS, BRICK, BRICK), tabs)[:5])
        return out.reshape(hidden.shape), dh.reshape(hidden.shape), dwq, dwk, dwv, dwo.reshape(w_out.shape)

    row_spec, head_spec = P(None, "cp", None), P("tp", None, None)
    query_spec = P(None, "tp", None)
    return jax.shard_map(local_program, mesh=mesh, in_specs=(row_spec, row_spec, query_spec, P(), P(), head_spec),
                         out_specs=(row_spec, row_spec, query_spec, P(), P(), head_spec), check_vma=False)
```

```python
import functools
import jax
import jax.numpy as jnp
from jax import lax
from jax.experimental import pallas as pl
from jax.experimental.pallas import tpu as pltpu
from jax.sharding import PartitionSpec as P

ROWS, DEPTH, LANE, TILE, BRICK, HALF_W = 1024, 4096, 128, 256, 512, 2048
CHIPS, HEADS, GROUPS = 4, 8, 8
VMEM_CAP = 66_000_000
MESH = pl.DeviceIdType.MESH
F32, BF16 = jnp.float32, jnp.bfloat16
NT = (((1,), (1,)), ((), ()))
NN = (((1,), (0,)), ((), ()))
TN = (((0,), (0,)), ((), ()))
ANY = pl.BlockSpec(memory_space=pl.ANY)
VM = pl.BlockSpec(memory_space=pltpu.VMEM)
DMA = pltpu.SemaphoreType.DMA


def dot(lhs, rhs, dims=NN):
    return lax.dot_general(lhs, rhs, dims, preferred_element_type=F32)


def cost(gigaflops):
    return pl.CostEstimate(flops=gigaflops * 10 ** 9, bytes_accessed=10 ** 8, transcendentals=0)


def talking(collective_id):
    return pltpu.CompilerParams(collective_id=collective_id, has_side_effects=True, vmem_limit_bytes=VMEM_CAP)


def by_row(reduce, tile):
    return reduce(tile, axis=1, keepdims=True)


def twice(tile):
    return jnp.concatenate([tile, tile], axis=0)


def win(index, size):
    start = index * size
    return pl.ds(start if isinstance(start, int) else pl.multiple_of(start, size), size)


def plane_peers(cp):
    x_of = lambda idx: idx + 2 - CHIPS * lax.rem(lax.div(idx, 2), 2)
    y_of = lambda idx: lax.rem(idx + CHIPS, HEADS)
    return x_of(cp), y_of(cp), x_of(y_of(cp)), cp + 1 - 2 * lax.rem(cp, 2)


def hand_over(src, dst, send_sem, recv_sem, tp, cp):
    return pltpu.make_async_remote_copy(src, dst, send_sem, recv_sem, device_id=(tp, cp), device_id_type=MESH)


def rope(tile, cos, sin):
    heads = [tile[:, lo:lo + LANE] for lo in range(0, tile.shape[1], LANE)]
    return [one * cos + pltpu.roll(one, LANE // 2, 1) * sin for one in heads]


def proj_kernel(q_scale, h_ref, g_ref, wq_ref, wo_ref, wk_ref, wv_ref, cos_ref, sin_ref,
                q_out, do_out, kv_out, hbuf, gbuf, wqbuf, wobuf, wkvbuf, qbuf, dobuf, kvbuf,
                load_sem, wkv_sem, osem, send_sem, recv_sem):
    tp, cp = lax.axis_index("tp"), lax.axis_index("cp")
    peers = plane_peers(cp)
    *others, partner = peers
    barrier = pltpu.get_barrier_semaphore()
    for peer in peers:
        pl.semaphore_signal(barrier, inc=1, device_id=(tp, peer), device_id_type=MESH)
    rows = [win(i, TILE) for i in range(CHIPS)]
    loads_h, loads_g, loads_wq, loads_wo = [
        [pltpu.make_async_copy(src.at[r], dst.at[r], load_sem.at[which, i]) for i, r in enumerate(rows)]
        for which, (src, dst) in enumerate(((h_ref, hbuf), (g_ref, gbuf), (wq_ref, wqbuf), (wo_ref, wobuf)))]
    loads_kv = [pltpu.make_async_copy(src, wkvbuf.at[:, win(i, LANE)], wkv_sem.at[i]) for i, src in enumerate((wk_ref, wv_ref))]
    for copy in loads_h[:1] + loads_kv + loads_h[1:]:
        copy.start()
    for copy in loads_h[:1] + loads_kv:
        copy.wait()
    for copy in loads_wq:
        copy.start()
    cos, sin = twice(cos_ref[...]), twice(sin_ref[...])
    sends, stored = [], []

    def share(i):
        piece = kv_out.at[cp, rows[i]]
        stored[i].wait()
        sends.append([hand_over(piece, piece, send_sem.at[n, i], recv_sem.at[n, i], tp, peer) for n, peer in enumerate(peers)])
        for copy in sends[i]:
            copy.start()

    for i, row in enumerate(rows):
        if i:
            loads_h[i].wait()
        kv = dot(hbuf[row, :], wkvbuf[...])
        kvbuf[row, win(0, LANE)] = rope(kv[:, :LANE], cos, sin)[0].astype(BF16)
        kvbuf[row, win(1, LANE)] = kv[:, LANE:].astype(BF16)
        stored.append(pltpu.make_async_copy(kvbuf.at[row], kv_out.at[cp, row], osem.at[2 + i]))
        stored[i].start()
        if i == 0:
            pl.semaphore_wait(barrier, len(peers))
        else:
            share(i - 1)
    share(CHIPS - 1)
    for copy in loads_wq:
        copy.wait()
    for copy in loads_g + loads_wo:
        copy.start()
    cos2, sin2 = twice(cos), twice(sin)

    @pl.loop(0, HEADS)
    def _(step):
        row, col = win(lax.div(step, CHIPS), BRICK), win(lax.rem(step, CHIPS), TILE)
        tile = dot(hbuf[row, :], wqbuf[col, :], NT)
        qbuf[row, col] = (jnp.concatenate(rope(tile, cos2, sin2), axis=1) * q_scale).astype(BF16)

    store_q = pltpu.make_async_copy(qbuf, q_out, osem.at[0])
    store_q.start()
    for copy in loads_g + loads_wo:
        copy.wait()
    passes = []

    def pass_on(i):
        for n, peer in enumerate(others):
            sends[i][n].wait_recv()
            piece = kv_out.at[peer, rows[i]]
            copy = hand_over(piece, piece, send_sem.at[CHIPS + n, i], recv_sem.at[CHIPS + n, i], tp, partner)
            copy.start()
            passes.append(copy)

    for half in range(2):
        @pl.loop(half * CHIPS, (half + 1) * CHIPS)
        def _(step):
            row, col = win(lax.div(step, CHIPS), BRICK), win(lax.rem(step, CHIPS), TILE)
            dobuf[row, col] = dot(gbuf[row, :], wobuf[col, :], NT).astype(BF16)

        pass_on(half)
    store_do = pltpu.make_async_copy(dobuf, do_out, osem.at[1])
    store_do.start()
    for i in range(2, CHIPS):
        pass_on(i)
    for group in sends:
        group[-1].wait_recv()
        for copy in group:
            copy.wait_send()
    for copy in passes:
        copy.wait()
    store_q.wait()
    store_do.wait()


def turn_kernel(w_ref, out_ref):
    out_ref[...] = w_ref[...].reshape(ROWS, ROWS).T


def turn(w):
    return pl.pallas_call(
        turn_kernel,
        name="turn",
        grid=(CHIPS,),
        out_shape=jax.ShapeDtypeStruct((ROWS, DEPTH), BF16),
        in_specs=[pl.BlockSpec((ROWS, HEADS, LANE), lambda i: (i, 0, 0))],
        out_specs=pl.BlockSpec((ROWS, ROWS), lambda i: (0, i)),
        compiler_params=pltpu.CompilerParams(vmem_limit_bytes=VMEM_CAP),
        cost_estimate=cost(1),
    )(w)


def projections(h, g, wq_t, wo2, wk, wv, cos_tab, sin_tab, q_scale):
    square = (ROWS, ROWS)
    kv_shape = (HEADS, ROWS, TILE)
    return pl.pallas_call(
        functools.partial(proj_kernel, q_scale),
        name="projections",
        out_shape=[jax.ShapeDtypeStruct(s, BF16) for s in (square, square, kv_shape)],
        in_specs=[ANY] * 6 + [VM] * 2,
        out_specs=[ANY] * 3,
        scratch_shapes=[pltpu.VMEM(s, BF16) for s in [(ROWS, DEPTH)] * 4 + [(DEPTH, TILE), square, square, (ROWS, TILE)]]
        + [DMA(s) for s in ((CHIPS, CHIPS), (2,), (6,), (7, CHIPS), (7, CHIPS))],
        compiler_params=talking(0),
        cost_estimate=cost(20),
    )(h, g, wq_t, wo2, wk, wv, cos_tab, sin_tab)


def attn_kernel(q_scale, q_ref, do_ref, kv_ref, mask_ref, cos_ref, sin_ref, o_ref, dq_ref, dkv_ref):
    keys = kv_ref[:, :, :LANE].reshape(ROWS, LANE)
    vals = kv_ref[:, :, LANE:].reshape(ROWS, LANE)
    cos, sin, mask = twice(cos_ref[...]), twice(sin_ref[...]), twice(mask_ref[...])
    sums = []
    for pair in range(CHIPS):
        cols = [win(2 * pair + i, LANE) for i in range(2)]
        q = jnp.concatenate([q_ref[:, c] for c in cols], axis=0)
        do = jnp.concatenate([do_ref[:, c] for c in cols], axis=0)
        scores = dot(q, keys, NT) + mask
        prob = jnp.exp(scores - by_row(jnp.max, scores))
        prob = prob * (1.0 / by_row(jnp.sum, prob))
        prob_b = prob.astype(BF16)
        out = dot(prob_b, vals).astype(BF16)
        delta = by_row(jnp.sum, do.astype(F32) * out.astype(F32))
        d_score = (prob * (dot(do, vals, NT) - delta)).astype(BF16)
        dq = dot(d_score, keys)
        dq = ((dq * cos - pltpu.roll(dq, LANE // 2, 1) * sin) * q_scale).astype(BF16)
        for i, c in enumerate(cols):
            o_ref[:, c] = out[i * LANE:(i + 1) * LANE]
            dq_ref[:, c] = dq[i * LANE:(i + 1) * LANE]
        sums.append((dot(q.T, d_score), dot(do.T, prob_b)))
    for kind, parts in enumerate(zip(*sums)):
        total = (parts[0] + parts[1]) + (parts[2] + parts[3])
        for j in range(HEADS):
            dkv_ref[j, kind] = total[:, j * LANE:(j + 1) * LANE]


def attention(q, do, kv, mask, cos_tab, sin_tab, q_scale):
    row_block = pl.BlockSpec((LANE, ROWS), lambda b: (b, 0))
    whole = lambda a: pl.BlockSpec(a.shape, lambda b: (0,) * a.ndim)
    return pl.pallas_call(
        functools.partial(attn_kernel, q_scale),
        name="attention",
        grid=(HEADS,),
        out_shape=[jax.ShapeDtypeStruct((ROWS, ROWS), BF16)] * 2 + [jax.ShapeDtypeStruct((HEADS, 2, TILE, BRICK), F32)],
        in_specs=[row_block, row_block, pl.BlockSpec((HEADS, LANE, TILE), lambda b: (0, b, 0)), whole(mask), whole(cos_tab), whole(sin_tab)],
        out_specs=[row_block, row_block, pl.BlockSpec((HEADS, 2, LANE, LANE), lambda b: (0, 0, lax.div(b, CHIPS), lax.rem(b, CHIPS)))],
        compiler_params=pltpu.CompilerParams(vmem_limit_bytes=VMEM_CAP),
        cost_estimate=cost(30),
    )(q, do, kv, mask, cos_tab, sin_tab)


def tables(cp):
    half = LANE // 2
    pos = cp * LANE + jnp.arange(LANE)
    inv_freq = 1.0 / jnp.power(10000.0, jnp.arange(half, dtype=F32) * (2.0 / LANE))
    ang = pos.astype(F32)[:, None] * inv_freq[None, :]
    cos, sin = jnp.cos(ang), jnp.sin(ang)
    mask = jnp.where(jnp.arange(ROWS)[None, :] <= pos[:, None], 0.0, -jnp.inf).astype(F32)
    return jnp.concatenate([cos.T, sin.T], axis=0), jnp.concatenate([cos, cos], axis=1), jnp.concatenate([-sin, sin], axis=1), mask


DKV, DWO, DWQ, DWKV = 0, (1, 2), (3, 4), 5
SETS, SLOTS = 6, 5
LEADS, EARLY = (3, 2), 3
LATER = (5, 6, 7, )
FAR_ROLES = (0, 2, 3)
PHASES, SOURCES = 2, len(FAR_ROLES)
INPUTS = ("o", "dq", "wo", "wq", "near", "mid", "far", "wk", "wv", "g", "h", "dkv", "tabs")
OUTPUTS = {"out": ((ROWS, DEPTH), BF16), "dh": ((ROWS, DEPTH), BF16), "dwo": ((ROWS, DEPTH), F32), "dwq": ((DEPTH, ROWS), F32),
           "dwkv": ((DEPTH, TILE), F32), "dkvb": ((ROWS, TILE), BF16), "wland": ((DEPTH, HALF_W), BF16),
           "pland": ((SETS, CHIPS, BRICK, BRICK), F32), "xland": ((SETS, PHASES, BRICK, BRICK), F32), "hland": ((SETS, PHASES, TILE, BRICK), F32), "zland": ((PHASES, BRICK, BRICK), F32)}
BUFFERS = {"abuf": ((ROWS, DEPTH + TILE), BF16), "wa": ((DEPTH, HALF_W), BF16), "wb": ((DEPTH, TILE), BF16), "wkv": ((DEPTH, TILE), BF16),
           "tile_a": ((LANE, HALF_W), BF16), "tile_b": ((ROWS, TILE), BF16), "keep": ((SLOTS, CHIPS, BRICK, BRICK), F32),
           "tmp": ((CHIPS, BRICK, BRICK), F32), "stage": ((PHASES, BRICK, BRICK), F32), "left": ((PHASES, ROWS, BRICK), BF16),
           "right": ((PHASES, ROWS, BRICK), BF16), "zbuf": ((BRICK, BRICK), F32)}
SEMS = {"load": (12,), "early": (CHIPS,), "held": (CHIPS,), "asend": (PHASES, GROUPS), "arecv": (PHASES, SOURCES, GROUPS), "wsend": (PHASES, GROUPS), "wrecv": (PHASES, SOURCES, GROUPS), "fsend": (PHASES, SOURCES), "frecv": (PHASES, SOURCES, GROUPS),
        "rsend": (PHASES, PHASES, PHASES, GROUPS), "rrecv": (PHASES, PHASES, GROUPS), "swsend": (SOURCES,), "swrecv": (SOURCES,), "dsend": (SETS, CHIPS), "drecv": (SETS, CHIPS),
        "xsend": (SETS, PHASES), "xrecv": (SETS, PHASES), "hsend": (SETS, PHASES), "hrecv": (SETS, PHASES), "zsend": (SOURCES,), "zrecv": (SOURCES,), "gsend": (SETS, 9), "grecv": (SETS, 9)}


class Exchange:
    def __init__(self, *refs):
        for name, ref in zip((*INPUTS, *OUTPUTS, *BUFFERS, *SEMS, "credit"), refs):
            setattr(self, name, ref)
        self.tp, self.cp = lax.axis_index("tp"), lax.axis_index("cp")
        self.core, self.chip = lax.rem(self.cp, 2), lax.div(self.cp, 2)
        self.x, self.y, self.diag, self.partner = plane_peers(self.cp)
        self.acts, self.weights, self.results = (self.o, self.dq), (self.wo, self.wq), (self.out, self.dh)

    def move(self, pairs):
        copies = [pltpu.make_async_copy(src, dst, self.load.at[i]) for i, (src, dst) in enumerate(pairs)]
        for copy in copies:
            copy.start()
        for copy in copies:
            copy.wait()


    def plane(self, phase, role):
        return CHIPS - 1 - role if phase else role

    def role(self, phase):
        return self.plane(phase, self.tp)

    def act_copy(self, phase, src, i, to):
        row = win(i, LANE)
        return hand_over(self.acts[phase].at[row], self.abuf.at[row, win(src, ROWS)], self.asend.at[phase, i],
                         self.arecv.at[phase, FAR_ROLES.index(src), i], to, self.cp)

    def w_copy(self, phase, src, n, to):
        rows = 2 * src + self.core
        return hand_over(self.weights[phase].at[win(self.core, BRICK), win(GROUPS + n, TILE)], self.wland.at[win(rows, BRICK), win(n, TILE)],
                         self.wsend.at[phase, n], self.wrecv.at[phase, FAR_ROLES.index(src), n], to, self.cp)

    def cross_copy(self, phase, src, n, core):
        place = self.wland.at[win(2 * src + core, BRICK), win(n, TILE)]
        slot = FAR_ROLES.index(src)
        return hand_over(place, place, self.fsend.at[phase, slot], self.frecv.at[phase, slot, n], self.tp, self.partner)

    def piece(self, phase, kind, idx):
        if kind:
            return self.results[phase].at[:, win(GROUPS + idx, TILE)]
        return self.results[phase].at[win(idx, LANE), win(0, HALF_W)]

    def result_copy(self, phase, kind, idx, way, to_role):
        piece = self.piece(phase, kind, idx)
        return hand_over(piece, piece, self.rsend.at[phase, way, kind, idx], self.rrecv.at[phase, kind, idx], self.plane(phase, to_role), self.cp)

    def ask_far(self, phase):
        pl.semaphore_signal(self.credit.at[phase], inc=1, device_id=(self.plane(phase, 3), self.cp), device_id_type=MESH)

    def multiply(self, phase, kind, idx):
        weight = self.weights[phase]

        def product(row, weights, col):
            total = dot(self.abuf[row, pl.ds(0, DEPTH)], weights)
            if phase:
                total = total + dot(self.abuf[row, pl.ds(DEPTH, TILE)], self.wkv[col, :], NT)
            return total.astype(BF16)

        if kind == 0:
            row = win(idx, LANE)
            for src in FAR_ROLES:
                self.act_copy(phase, src, idx, self.plane(phase, src)).wait_recv()
            self.ask_far(phase)

            @pl.loop(0, CHIPS)
            def _(i):
                col = win(i, BRICK)
                self.tile_a[:, col] = product(row, self.wa[:, col], col)
        else:
            for src in FAR_ROLES:
                self.cross_copy(phase, src, idx, 1 - self.core).wait_recv()
                self.cross_copy(phase, src, idx, self.core).wait_send()
            pairs = [(self.wland.at[win(src, ROWS), win(idx, TILE)], self.wb.at[win(src, ROWS)]) for src in FAR_ROLES]
            pairs.append((weight.at[:, win(GROUPS + idx, TILE)], self.wb.at[win(1, ROWS)]))
            self.move(pairs)

            @pl.loop(0, CHIPS)
            def _(i):
                row = win(i, TILE)
                self.tile_b[row, :] = product(row, self.wb[...], win(GROUPS + idx, TILE))

        self.move([(self.tile_b if kind else self.tile_a, self.piece(phase, kind, idx))])
        for way, to_role in enumerate((0, 2)):
            self.result_copy(phase, kind, idx, way, to_role).start()

    def swap_weights(self, phase, idx):
        @pl.when(self.role(phase) == 1)
        def _():
            for src in FAR_ROLES:
                self.w_copy(phase, src, idx, self.plane(phase, src)).wait_recv()
                self.cross_copy(phase, src, idx, self.core).start()

            @pl.when(idx < GROUPS - LEADS[phase])
            def _():
                self.ask_far(phase)

    def group(self, phase, kind, idx):
        role = self.role(phase)

        @pl.when(role == 0)
        def _():
            self.result_copy(phase, kind, idx, 0, 1).wait_recv()

        @pl.when(role == 1)
        def _():
            self.multiply(phase, kind, idx)

        @pl.when(role == 2)
        def _():
            self.result_copy(phase, kind, idx, 0, 1).wait_recv()
            self.result_copy(phase, kind, idx, 0, 3).start()

        item = idx + LEADS[phase]

        @pl.when((role == 3) & ((item < GROUPS) | (kind == 0)))
        def _():
            pl.semaphore_wait(self.credit.at[phase], 1)

            @pl.when((item < GROUPS) & (kind == 0))
            def _():
                self.act_copy(phase, 3, item, self.plane(phase, 1)).start()

            @pl.when((item >= GROUPS) | (kind == 1))
            def _():
                self.w_copy(phase, 3, lax.rem(item, GROUPS), self.plane(phase, 1)).start()

    def feed(self, phase, src, acts, weights):
        @pl.when(self.role(phase) == src)
        def _():
            for i in acts:
                self.act_copy(phase, src, i, self.plane(phase, 1)).start()
            for n in weights:
                self.w_copy(phase, src, n, self.plane(phase, 1)).start()

    def start_line(self):
        for phase in range(PHASES):
            @pl.when(self.role(phase) == 1)
            def _():
                swaps = []
                for i, (half, src) in enumerate(zip((self.near, self.mid, self.far), FAR_ROLES)):
                    swaps.append(hand_over(half, self.wa.at[win(2 * src + self.core, BRICK)], self.swsend.at[i], self.swrecv.at[i], self.tp, self.partner))
                    swaps[i].start()
                pairs = [(half, self.wa.at[win(2 * src + self.core, BRICK)]) for half, src in zip((self.near, self.mid, self.far), FAR_ROLES)]
                pairs.append((self.weights[phase].at[:, win(0, HALF_W)], self.wa.at[win(1, ROWS)]))
                pairs.append((self.acts[phase], self.abuf.at[:, win(1, ROWS)]))
                pairs += [(src, self.wkv.at[:, win(i, LANE)]) for i, src in enumerate((self.wk, self.wv))]
                self.move(pairs)

    def end_swap(self):
        @pl.when((self.tp == 1) | (self.tp == 2))
        def _():
            for i, (half, src) in enumerate(zip((self.near, self.mid, self.far), FAR_ROLES)):
                hand_over(half, self.wa.at[win(2 * src + 1 - self.core, BRICK)], self.swsend.at[i], self.swrecv.at[i], self.tp, self.partner).wait()

    def end_line(self):
        for phase in range(PHASES):
            role = self.role(phase)
            for kind in range(PHASES):
                @pl.when(role == 1)
                def _():
                    @pl.loop(0, GROUPS)
                    def _(idx):
                        for way, to_role in enumerate((0, 2)):
                            self.result_copy(phase, kind, idx, way, to_role).wait_send()

                @pl.when(role == 2)
                def _():
                    @pl.loop(0, GROUPS)
                    def _(idx):
                        self.result_copy(phase, kind, idx, 0, 3).wait_send()

                @pl.when(role == 3)
                def _():
                    @pl.loop(0, GROUPS)
                    def _(idx):
                        self.result_copy(phase, kind, idx, 0, 2).wait_recv()

            for src in FAR_ROLES:
                @pl.when(role == src)
                def _():
                    for i in range(GROUPS):
                        self.act_copy(phase, src, i, self.plane(phase, 1)).wait_send()
                        self.w_copy(phase, src, i, self.plane(phase, 1)).wait_send()


    def brick(self, which, ref):
        return ref.at[:, pl.ds(0, TILE)] if which == DWKV else ref

    def pair_copy(self, kind, i, src, which=None):
        which = kind if which is None else which
        return hand_over(src, self.brick(kind, self.pland.at[which, i]), self.dsend.at[which, i], self.drecv.at[which, i], self.tp, self.partner)

    def chip_copies(self, which):
        return [hand_over(self.brick(which, self.keep.at[which % SLOTS, lax.div(peer, 2)]), self.brick(which, self.xland.at[which, n]),
                          self.xsend.at[which, n], self.xrecv.at[which, n], self.tp, peer) for n, peer in enumerate((self.x, self.y))]

    def half_copies(self, which):
        block = self.brick(which, self.keep.at[which % SLOTS, lax.div(self.diag, 2)])
        return [hand_over(block.at[win(n, TILE)], self.brick(which, self.hland.at[which, n]),
                          self.hsend.at[which, n], self.hrecv.at[which, n], self.tp, peer) for n, peer in enumerate((self.x, self.y))]

    def own_blocks(self):
        return [pltpu.make_async_copy(self.dkv.at[2 * i + self.core], self.keep.at[0, i], self.held.at[i]) for i in range(CHIPS)]

    def hand_dkv(self):
        for i in range(CHIPS):
            self.pair_copy(DKV, i, self.dkv.at[2 * i + 1 - self.core]).start()
        for copy in self.own_blocks():
            copy.start()
        self.fetch(0)

    def fetch(self, part):
        half, i = win(lax.rem(lax.div(part, CHIPS), 2), BRICK), lax.rem(part, CHIPS)
        narrow = pl.ds(0, TILE)
        for n, block in enumerate((2 * i + 1 - self.core, 2 * i + self.core)):
            block = win(block, BRICK)
            right = self.right.at[n]
            for kind, pair in enumerate((((self.o.at[:, half], self.left.at[n]), (self.g.at[:, block], right)),
                                         ((self.h.at[:, block], self.left.at[n]), (self.dq.at[:, half], right)),
                                         ((self.h.at[:, block], self.left.at[n]), (self.dkvb, right.at[:, narrow])))):
                @pl.when(lax.div(part, 2 * CHIPS) == kind)
                def _():
                    for m, (src, dst) in enumerate(pair):
                        pltpu.make_async_copy(src, dst, self.early.at[2 * n + m]).start()

    def make(self, part, which=None):
        kind, i = which, lax.rem(part, CHIPS)
        which = 1 + lax.div(part, CHIPS) if which is None else which
        col = pl.ds(0, BRICK if kind is None else TILE)
        slot = self.stage.at[lax.rem(part, 2), :, col]

        before = part - 2

        @pl.when((before >= 0) & (before < PARTS))
        def _():
            self.pair_copy(None, lax.rem(before, CHIPS), self.stage.at[0], 1 + lax.div(before, CHIPS)).wait_send()

        @pl.when(before >= PARTS)
        def _():
            self.pair_copy(DWKV, before - PARTS, self.brick(DWKV, self.stage.at[0])).wait_send()

        for n, dst in enumerate((slot, self.keep.at[lax.rem(which, SLOTS), i, :, col])):
            left, right = self.left.at[n], self.right.at[n, :, col]
            for m, factor in enumerate((left, right)):
                pltpu.make_async_copy(self.h.at[:, col] if m else self.h.at[:, win(0, BRICK)], factor, self.early.at[2 * n + m]).wait()
            dst[...] = dot(left[...], right[...], TN)
            if n == 0:
                self.pair_copy(kind, i, slot, which).start()

        @pl.when((part != PARTS - 1) & (part != PARTS + CHIPS - 1))
        def _():
            self.fetch(part + 1)

    def total(self, which, count, add):
        @pl.loop(0, count * HEADS)
        def _(step):
            add(lax.div(step, HEADS), win(lax.rem(step, HEADS), LANE // 2))

    def add_pair(self, which):
        keep = self.keep.at[which % SLOTS]
        landed = [self.brick(which, self.pland.at[which, i]) for i in range(CHIPS)]
        for i in range(CHIPS):
            self.pair_copy(which, i, landed[i]).wait_recv()
        for i in range({DKV: 0, DWKV: 2}.get(which, CHIPS), CHIPS):
            self.pair_copy(which, i, landed[i]).wait_send()
        if which == DKV:
            for copy in self.own_blocks():
                copy.wait()
        self.move([(landed[i], self.brick(which, self.tmp.at[i])) for i in range(CHIPS)])
        col = pl.ds(0, TILE if which == DWKV else BRICK)

        def add(i, row):
            keep[i, row, col] = keep[i, row, col] + self.tmp[i, row, col]

        self.total(which, CHIPS, add)
        for copy in self.half_copies(which):
            copy.start()

    def relay(self, which):
        for copy in self.half_copies(which):
            copy.wait()
        self.move([(self.brick(which, self.hland.at[which, n]), self.brick(which, self.tmp.at[n, win(0, TILE)])) for n in range(2)])
        col = pl.ds(0, TILE if which == DWKV else BRICK)
        for n, peer in enumerate((self.y, self.x)):
            block = self.keep.at[which % SLOTS, lax.div(peer, 2)]
            for step in range(CHIPS):
                row, src = win(CHIPS * n + step, LANE // 2), win(step, LANE // 2)
                block[row, col] = block[row, col] + self.tmp[n, src, col]
        for copy in self.chip_copies(which):
            copy.start()

    def place(self, which, owner):
        if which in DWO:
            return self.dwo.at[win(which - DWO[0], BRICK), win(owner, BRICK)]
        if which in DWQ:
            return self.dwq.at[win(owner, BRICK), win(which - DWQ[0], BRICK)]
        return self.dwkv.at[win(owner, BRICK)]

    def share_copy(self, which, kind):
        owner = (self.cp, self.cp, self.cp, self.x, self.y, self.y, self.x, self.diag, self.diag)[kind]
        to = (self.x, self.y, self.partner, self.partner, self.partner, self.x, self.y, self.partner, self.partner)[kind]
        place = self.place(which, owner)
        if kind > 4:
            place = place.at[win((kind + 1) % 2, TILE)]
        return hand_over(place, place, self.gsend.at[which, kind], self.grecv.at[which, kind], self.tp, to)

    def shared_place(self, which, kind):
        mate = lambda idx: plane_peers(idx)[-1]
        owner = (self.x, self.y, self.partner, mate(self.x), mate(self.y), self.diag, self.diag, mate(self.diag), mate(self.diag))[kind]
        place = self.place(which, owner)
        if kind > 4:
            place = place.at[win((kind + 1) % 2, TILE)]
        return hand_over(place, place, self.gsend.at[which, kind], self.grecv.at[which, kind], self.tp, self.partner)

    def add_chips(self, which):
        copies = self.chip_copies(which)
        for copy in copies:
            copy.wait()
        self.move([(self.brick(which, self.xland.at[which, n]), self.brick(which, self.tmp.at[n])) for n in range(len(copies))])
        col = pl.ds(0, TILE if which == DWKV else BRICK)
        own = self.keep.at[which % SLOTS, self.chip]

        def add(_, row):
            own[row, col] = own[row, col] + (self.tmp[0, row, col] + self.tmp[1, row, col])

        self.total(which, 1, add)
        if which == DKV:
            self.total(which, 1, self.keep_z)
            for end, inner in ((0, 1), (3, 2)):
                @pl.when(self.tp == end)
                def _():
                    self.z_copy(0, inner).start()
            return
        self.move([(self.brick(which, own), self.place(which, self.cp))])
        for kind in range(3):
            self.share_copy(which, kind).start()

    def pass_on(self, which):
        for kind in range(PHASES):
            self.shared_place(which, kind).wait_recv()
        for kind in (5, 6, 3, 4):
            self.share_copy(which, kind).start()

    def pass_diagonal(self, which):
        for kind in (5, 6):
            self.shared_place(which, kind).wait_recv()
        for kind in (7, 8):
            self.share_copy(which, kind).start()

    def end_share(self, which):
        for kind in (2, 3, 4, 7, 8):
            self.shared_place(which, kind).wait_recv()
        for kind in range(9):
            self.share_copy(which, kind).wait_send()


    def keep_z(self, _, row):
        self.zbuf[row] = self.keep[0, self.chip, row]

    def z_copy(self, slot, to):
        return hand_over(self.zbuf, self.zland.at[slot], self.zsend.at[slot], self.zrecv.at[slot], to, self.cp)

    def z_result(self, slot, to):
        return hand_over(self.dkvb, self.dkvb, self.zsend.at[slot], self.zrecv.at[2], to, self.cp)

    def meet(self):
        for inner in (1, 2):
            @pl.when(self.tp == inner)
            def _():
                self.z_copy(0, CHIPS - 1 - inner).wait_recv()
                self.move([(self.zland.at[0], self.tmp.at[0])])

                def add(_, row):
                    self.zbuf[row] = self.zbuf[row] + self.tmp[0, row]

                self.total(DKV, 1, add)
                if inner == 2:
                    self.z_copy(1, 1).start()
                    self.feed(0, 2, (), LATER)

    def settle(self):
        half = LANE // 2

        @pl.when(self.tp == 1)
        def _():
            self.z_copy(1, 2).wait_recv()
            self.move([(self.zland.at[1], self.tmp.at[0]), (self.tabs, self.tmp.at[1, win(0, LANE), win(0, LANE)])])
            for b in range(HEADS):
                cos, sin = self.tmp[1, win(0, half), win(0, LANE)], self.tmp[1, win(1, half), win(0, LANE)]
                for kind in range(PHASES):
                    row, col = win(2 * kind + b // CHIPS, LANE), win(b % CHIPS, LANE)
                    part = self.zbuf[row, col] + self.tmp[0, row, col]
                    if kind == 0:
                        low, high = part[:half], part[half:]
                        part = jnp.concatenate([low * cos + high * sin, high * cos - low * sin], axis=0)
                    self.abuf[win(b, LANE), win(DEPTH // LANE + kind, LANE)] = part.T.astype(BF16)
            self.move([(self.abuf.at[:, pl.ds(DEPTH, TILE)], self.dkvb)])
            self.z_result(2, 2).start()
            self.z_result(0, 0).start()

    def take(self):
        @pl.when(self.tp == 2)
        def _():
            self.z_result(2, 1).wait_recv()
            self.z_result(2, 3).start()
            self.move([(self.dkvb, self.abuf.at[:, pl.ds(DEPTH, TILE)])])

    def get_result(self):
        for end in (0, 3):
            @pl.when(self.tp == end)
            def _():
                self.z_result(2, 1).wait_recv()
                self.z_copy(0, 1).wait_send()

        @pl.when(self.tp == 1)
        def _():
            self.z_result(0, 0).wait_send()

        @pl.when(self.tp == 2)
        def _():
            self.z_copy(1, 1).wait_send()

        @pl.when((self.tp == 1) | (self.tp == 2))
        def _():
            self.z_result(2, 3).wait_send()


STEPS = {"add_pair": ((1, 3, 5, 9, 9, 22), (2, 5, 5, 7, 11, 27)),
         "relay": ((2, 5, 11, 12, 14, 26), (3, 9, 14, 11, 12, 28)),
         "add_chips": ((9, 9, 14, 21, 23, 30), (6, 12, 21, 21, 16, 30)),
         "pass_on": ((19, 25, 27, 26, 31), (17, 25, 29, 20, 31)),
         "pass_diagonal": ((27, 28, 30, 31, 31), (21, 29, 31, 24, 31))}
ONCE = {"hand_dkv": 0, "meet": 10, "get_result": 17}
PARTS, LATE = 16, (18, 18)
TURN, TURNS, NEAR, MID = 13, (13, 16, 13, 14), (10, 20), (16, 16)


def exchange_kernel(*refs):
    dev = Exchange(*refs)
    barrier = pltpu.get_barrier_semaphore()
    for step in range(1, CHIPS):
        pl.semaphore_signal(barrier, inc=1, device_id=(lax.rem(dev.tp + step, CHIPS), dev.cp), device_id_type=MESH)
    for peer in plane_peers(dev.cp):
        pl.semaphore_signal(barrier, inc=1, device_id=(dev.tp, peer), device_id_type=MESH)
    pl.semaphore_wait(barrier, 7)
    blocks = range(GROUPS)
    dev.feed(0, 3, blocks[:LEADS[0]], ())
    dev.feed(0, 0, blocks[:1], ())
    for i in blocks[1:]:
        dev.feed(0, 0, (i,), ())
        if i <= LEADS[1]:
            dev.feed(1, 3, (i - 1,), ())
    dev.feed(0, 0, (), blocks)
    dev.feed(0, 2, blocks, blocks[:GROUPS - len(LATER)])
    dev.feed(1, 2, blocks[:EARLY], ())
    dev.start_line()
    dev.end_swap()
    busy = dev.tp == 2

    @pl.loop(0, CHIPS * GROUPS)
    def _(now):
        turn = TURNS[0]
        for plane, own_turn in enumerate(TURNS):
            turn = jnp.where(dev.tp == plane, own_turn, turn)
        ahead = now - turn
        job = jnp.where(lax.rem(ahead, 2) == 0, 2 * GROUPS, turn) + lax.div(ahead, 2)
        job = jnp.where((ahead >= 0) & (now + turn < CHIPS * GROUPS), job, now)
        idx = lax.rem(job, GROUPS)
        spans = [(lax.div(job, GROUPS) == 2 * phase + kind, phase, kind) for phase in range(PHASES) for kind in range(PHASES)]

        for slots, src, acts in ((NEAR, 0, blocks), (MID, 2, blocks[EARLY:])):
            for slot, operands in zip(slots, ((acts, ()), ((), blocks))):
                @pl.when(now == slot)
                def _():
                    dev.feed(1, src, *operands)

        @pl.when(now == TURN)
        def _():
            dev.settle()
            dev.take()

        for here, phase, kind in spans:
            @pl.when(here)
            def _():
                if kind:
                    dev.swap_weights(phase, idx)
                else:
                    dev.group(phase, kind, idx)

        for step, at in ONCE.items():
            @pl.when(now == at)
            def _():
                getattr(dev, step)()

        for step, (early, late) in STEPS.items():
            for which in range(SETS - len(late), SETS):
                @pl.when(now == jnp.where(busy, early[which - SETS], late[which - SETS]))
                def _():
                    getattr(dev, step)(which)

        @pl.loop(jnp.clip(2 * now - 2, 0, PARTS), jnp.clip(2 * now, 0, PARTS))
        def _(part):
            dev.make(part)

        late = now - jnp.where(busy, *LATE)

        @pl.when(late == 0)
        def _():
            dev.fetch(PARTS)

        @pl.when((late >= 0) & (late < CHIPS))
        def _():
            dev.make(late + PARTS, DWKV)

        for here, phase, kind in spans:
            if kind:
                @pl.when(here)
                def _():
                    dev.group(phase, kind, idx)

    for which in range(1, SETS):
        dev.end_share(which)
    dev.end_line()


def exchange(*operands):
    return pl.pallas_call(
        exchange_kernel,
        name="exchange",
        out_shape=[jax.ShapeDtypeStruct(*spec) for spec in OUTPUTS.values()],
        in_specs=[ANY] * len(operands),
        out_specs=[ANY] * len(OUTPUTS),
        scratch_shapes=[pltpu.VMEM(*spec) for spec in BUFFERS.values()] + [DMA(shape) for shape in SEMS.values()] + [pltpu.SemaphoreType.REGULAR((2,))],
        compiler_params=talking(1),
        cost_estimate=cost(300),
    )(*operands)


def finish_kernel(out_ref, dh_ref, dwo_ref, dwq_ref, dwkv_ref, out, dh, dwo, dwq, dwk, dwv):
    out[...] = out_ref[...]
    dh[...] = dh_ref[...]
    dwo[...] = dwo_ref[...]
    dwq[...] = dwq_ref[...].reshape(dwq.shape)
    dwk[...] = dwkv_ref[:, :LANE]
    dwv[...] = dwkv_ref[:, LANE:]


def finish(*arrays, steps=HEADS):
    heads = (DEPTH, HEADS, LANE)
    shapes = [(arrays[0].shape, BF16), (arrays[1].shape, BF16), (arrays[2].shape, F32), (heads, F32), ((DEPTH, LANE), F32), ((DEPTH, LANE), F32)]
    block = lambda shape: pl.BlockSpec((shape[0] // steps, *shape[1:]), lambda i: (i,) + (0,) * (len(shape) - 1))
    return pl.pallas_call(
        finish_kernel,
        name="finish",
        grid=(steps,),
        out_shape=[jax.ShapeDtypeStruct(*spec) for spec in shapes],
        in_specs=[block(a.shape) for a in arrays],
        out_specs=[block(shape) for shape, _ in shapes],
        compiler_params=pltpu.CompilerParams(vmem_limit_bytes=VMEM_CAP),
        cost_estimate=cost(1),
    )(*arrays)


def solution(mesh):
    def local_program(hidden, grad_out, w_query, w_key, w_value, w_out):
        tp, cp = lax.axis_index("tp"), lax.axis_index("cp")
        h, g = hidden.reshape(ROWS, DEPTH), grad_out.reshape(ROWS, DEPTH)
        q_scale = LANE ** -0.5
        tabs, cos_tab, sin_tab, mask = tables(cp)
        wo2 = w_out.reshape(ROWS, DEPTH)
        wq_t = turn(w_query)
        wo_half, wq_half = [lax.dynamic_slice(w, (lax.rem(cp, 2) * BRICK, 0), (BRICK, HALF_W)) for w in (wo2, wq_t)]
        one_way, other_way = jnp.where(tp <= 1, wo_half, wq_half), jnp.where(tp <= 1, wq_half, wo_half)
        near = lax.ppermute(one_way, "tp", [(0, 1), (3, 2)])
        mid = lax.ppermute(other_way, "tp", [(2, 1), (1, 2)])
        far = lax.ppermute(other_way, "tp", [(3, 1), (0, 2)])
        q, d_o, kv = projections(h, g, wq_t, wo2, w_key, w_value, cos_tab, sin_tab, q_scale)
        o, dq, dkv = attention(q, d_o, kv, mask, cos_tab, sin_tab, q_scale)
        out, dh, dwo, dwq, dwk, dwv = finish(*exchange(o, dq, wo2, wq_t, near, mid, far, w_key, w_value, g, h, dkv.reshape(HEADS, BRICK, BRICK), tabs)[:5])
        return out.reshape(hidden.shape), dh.reshape(hidden.shape), dwq, dwk, dwv, dwo.reshape(w_out.shape)

    row_spec, head_spec = P(None, "cp", None), P("tp", None, None)
    query_spec = P(None, "tp", None)
    return jax.shard_map(local_program, mesh=mesh, in_specs=(row_spec, row_spec, query_spec, P(), P(), head_spec),
                         out_specs=(row_spec, row_spec, query_spec, P(), P(), head_spec), check_vma=False)
```
